8 devices in a mesh: rep: 2 (over y, z), dp: 4 (over x, core).
Axes of the slice: x: 2, y: 2, z: 1, core: 2. Of those that a mesh axis runs over, the one named last changes fastest.
Arguments:
- x: bfloat16 [8, 2048, 768], P(('rep', 'dp')), parts along dimension 0
- dy: bfloat16 [8, 2048, 768], P(('rep', 'dp')), parts along dimension 0
- w_gate: bfloat16 [2, 768, 3072], P(None, 'dp')
- w_up: bfloat16 [2, 768, 3072], P(None, 'dp')
- w_down: bfloat16 [2, 3072, 768], P(None, 'dp')
- m_w_gate: float32 [2, 768, 3072], P(None, 'dp')
- m_w_up: float32 [2, 768, 3072], P(None, 'dp')
- m_w_down: float32 [2, 3072, 768], P(None, 'dp')
- v_w_gate: float32 [2, 768, 3072], P(None, 'dp')
- v_w_up: float32 [2, 768, 3072], P(None, 'dp')
- v_w_down: float32 [2, 3072, 768], P(None, 'dp')
Outputs:
- output 1: bfloat16 [4, 768, 3072], P('rep', 'dp'), parts along dimension 0
- output 2: bfloat16 [4, 768, 3072], P('rep', 'dp'), parts along dimension 0
- output 3: bfloat16 [4, 3072, 768], P('rep', 'dp'), parts along dimension 0
- output 4: float32 [4, 768, 3072], P('rep', 'dp'), parts along dimension 0
- output 5: float32 [4, 768, 3072], P('rep', 'dp'), parts along dimension 0
- output 6: float32 [4, 3072, 768], P('rep', 'dp'), parts along dimension 0
- output 7: float32 [4, 768, 3072], P('rep', 'dp'), parts along dimension 0
- output 8: float32 [4, 768, 3072], P('rep', 'dp'), parts along dimension 0
- output 9: float32 [4, 3072, 768], P('rep', 'dp'), parts along dimension 0
There are 2 independent parts. The reference program is written for one: setup_inputs(seed, part) draws one part's arguments, and reference() takes and returns one part's arrays. A program takes and returns all parts, laid end to end along the dimension named above; an argument that names none is the same for every part.
All inputs are finite; a program needn't handle non-finite values.
Results may differ from the reference program's by a relative error of at most 0.022.
Values are sent between devices in bfloat16 or wider.
A program may use at most 2 GiB of HBM per device.

```python
import jax
import jax.numpy as jnp
from jax import lax

SEQUENCES = 4
TOKENS = 2048
D = 768
FF = 3072
LAYERS = 2
NAMES = ("w_gate", "w_up", "w_down")
SHAPES = {"w_gate": (LAYERS, D, FF), "w_up": (LAYERS, D, FF), "w_down": (LAYERS, FF, D)}


def bump(key, n, height):
    away = (jnp.arange(n, dtype=jnp.int32) - jax.random.randint(key, (), 0, n, jnp.int32)) % n
    return jnp.where(away < n // 8, height, 1.0)


def together(key, own, strength):
    shared = jax.random.normal(key, own.shape[1:], jnp.float32)
    return (own + strength * shared) * lax.rsqrt(1 + strength * strength)


def setup_inputs(seed: int = 0, part: int = 0) -> dict:
    kx, kdy, ka, kb, kz, kf, kh, kl, *keys = jax.random.split(jax.random.key(seed), 8 + 3 * len(NAMES))
    kx, kdy, ka, kb = (jax.random.fold_in(k, part) for k in (kx, kdy, ka, kb))
    kw, km, kv = (keys[i::3] for i in range(3))
    shape = (SEQUENCES, TOKENS, D)
    much_x, much_dy = jax.random.uniform(kz, (2,), jnp.float32, 0.0, 1.0)
    loud = 2.0 ** jax.random.uniform(jax.random.fold_in(kz, 1), (), jnp.float32, -1.0, 2.0)
    layers = 2.0 ** jax.random.uniform(kl, (LAYERS, 1, 1), jnp.float32, -1.0, 1.0)
    x = together(ka, jax.random.normal(kx, shape, jnp.float32), much_x) * bump(kf, D, 4.0)
    dy = together(kb, jax.random.normal(kdy, shape, jnp.float32), much_dy)
    drawn = {"x": x.astype(jnp.bfloat16), "dy": (loud * dy * (SEQUENCES * TOKENS) ** -0.5).astype(jnp.bfloat16)}
    for key, name in zip(kw, NAMES, strict=True):
        w = jax.random.normal(key, SHAPES[name], jnp.float32) * SHAPES[name][1] ** -0.5
        drawn[name] = (w * {"w_gate": 1.0, "w_up": bump(kh, FF, 4.0), "w_down": layers}[name]).astype(jnp.bfloat16)
    for key, name in zip(km, NAMES, strict=True):
        drawn[f"m_{name}"] = 0.1 * jax.random.normal(key, SHAPES[name], jnp.float32)
    for key, name in zip(kv, NAMES, strict=True):
        drawn[f"v_{name}"] = jax.random.uniform(key, SHAPES[name], jnp.float32, 0.005, 0.015)
    return drawn


def matmul(a, w):
    return jnp.dot(a, w, preferred_element_type=jnp.float32).astype(jnp.bfloat16)


def normed(h):
    wide = h.astype(jnp.float32)
    scale = lax.rsqrt(jnp.mean(wide**2, -1, keepdims=True) + 1e-6)
    return (wide * scale).astype(jnp.bfloat16)


def layer(h, w):
    a = normed(h)
    gate = jnp.dot(a, w["w_gate"], preferred_element_type=jnp.float32)
    up = jnp.dot(a, w["w_up"], preferred_element_type=jnp.float32)
    return h + matmul((jax.nn.silu(gate) * up).astype(jnp.bfloat16), w["w_down"])


def adamw(w, m, v, g):
    m = 0.9 * m + 0.1 * g
    v = 0.95 * v + 0.05 * g * g
    step = m * lax.rsqrt(v + 1e-8) + 0.1 * w
    return (w - 0.02 * step).astype(jnp.bfloat16), m, v


def clipped(gradients, sum_of_squares, count):
    factor = jnp.minimum(1.0, 0.5 * lax.rsqrt(sum_of_squares / count + 1e-30))
    return [g * factor for g in gradients]


def stack(weights, h):
    return lax.scan(lambda h, w: (layer(h, w), None), h, weights)[0]


def reference(x, dy, w_gate, w_up, w_down, m_w_gate, m_w_up, m_w_down, v_w_gate, v_w_up, v_w_down):
    weights = dict(zip(NAMES, (w_gate, w_up, w_down), strict=True))

    def take(so_far, sequence):
        h, by_y = sequence
        _, back = jax.vjp(lambda w: stack(w, h), weights)
        return jax.tree.map(lambda total, term: total + term.astype(jnp.float32), so_far, back(by_y)[0]), None

    none_yet = {name: jnp.zeros(w.shape, jnp.float32) for name, w in weights.items()}
    by_weights, _ = lax.scan(take, none_yet, (x, dy))
    gradients = [by_weights[name].astype(jnp.bfloat16).astype(jnp.float32) for name in NAMES]
    gradients = clipped(gradients, sum(jnp.sum(g * g) for g in gradients), sum(g.size for g in gradients))
    new = [
        adamw(w.astype(jnp.float32), m, v, g)
        for w, m, v, g in zip((w_gate, w_up, w_down), (m_w_gate, m_w_up, m_w_down), (v_w_gate, v_w_up, v_w_down), gradients, strict=True)
    ]
    return tuple(one[which] for which in range(3) for one in new)
```

```python
import functools

import jax
import jax.numpy as jnp
from jax import lax
from jax.experimental import pallas as pl
from jax.experimental.pallas import tpu as pltpu
from jax.sharding import PartitionSpec as P

T, D, FF, L = 2048, 768, 3072, 2
C = 768
TM = 512
RB = D // 4
RH = RB // 2
DH = C // 2
COUNT = 3 * L * D * FF
bf16, f32 = jnp.bfloat16, jnp.float32
NT = (((1,), (1,)), ((), ()))
TN = (((0,), (0,)), ((), ()))
MESH = pl.DeviceIdType.MESH


def dot(a, b, dims=(((1,), (0,)), ((), ()))):
    return lax.dot_general(a, b, dims, preferred_element_type=f32)


def scale_of(wide):
    return lax.rsqrt(jnp.mean(wide * wide, -1, keepdims=True) + 1e-6)


def step_kernel(
    x_hbm, dy_hbm, wg, wu, wd,
    gg_hbm, gu_hbm, gd_hbm, fac, all_g, all_u, all_d, p0_hbm, rd2_hbm, rx_hbm, own_d, rd_d, rx_d,
    h, a0, a1, do, acc, acc_gu, acc_d, w_gu, w_d, act_s, dgu_s, sg, sd, rd3, rd3d, sx, sxd, ssq, ss, ss_src,
    ag_s, ag_r, pe_s, pe_r, ld, wsem, d_s, d_r3, d_r3d, d_r2, d_rd, keep, x_s, x_r, xd_s, xd_r, fsem, fout, ss_s, ss_r,
):
    y, i = lax.axis_index("rep"), lax.axis_index("dp")
    xx, c = i // 2, i % 2
    ix, ip, iq = (1 - xx) * 2 + c, xx * 2 + 1 - c, (1 - xx) * 2 + 1 - c
    at_x, at_p, at_q, at_y = (y, ix), (y, ip), (y, iq), (1 - y, i)

    def remote(src, dst, send, recv, to):
        return pltpu.make_async_remote_copy(
            src_ref=src, dst_ref=dst, send_sem=send, recv_sem=recv, device_id=to, device_id_type=MESH
        )

    def chunk(k):
        return (2 * xx + k) % 4

    def chunk_there(k):
        return (2 * (1 - xx) + k) % 4

    def cols(j):
        return pl.ds(pl.multiple_of(j * C, C), C)

    def rows(start, size):
        return pl.ds(pl.multiple_of(start, 32), size)

    barrier = pltpu.get_barrier_semaphore()
    for other in (at_x, at_p, at_q, at_y):
        pl.semaphore_signal(barrier, inc=1, device_id=other, device_id_type=MESH)
    load_x = pltpu.make_async_copy(x_hbm, h, ld.at[0])
    load_dy = pltpu.make_async_copy(dy_hbm, do, ld.at[1])
    load_x.start()
    load_dy.start()
    pl.semaphore_wait(barrier, 4)

    def region(l, p, src, half, j):
        if p == 8:
            return all_d.at[l, rows(C * src + DH * half, DH), :]
        return (all_g, all_u)[p % 2].at[l, rows(RB * src + RH * half, RH), cols(j)]

    def mine(l, p, src, half):
        return region(l, p, src, half, chunk(p // 2))

    def send_x(l, p):
        if p == 8:
            src = wd.at[l, rows(DH * y, DH), :]
        else:
            src = (wg, wu)[p % 2].at[l, rows(RH * y, RH), cols(chunk_there(p // 2))]
        return remote(src, region(l, p, i, y, chunk_there(p // 2)), ag_s.at[l, p, 0], ag_r.at[l, p, 0], at_x)

    def forward_x(l, *ps):
        for p in ps:
            r = mine(l, p, ix, y)
            remote(r, r, ag_s.at[l, p, 0], ag_r.at[l, p, 0], at_x).wait_recv()
            remote(r, r, ag_s.at[l, p, 1], ag_r.at[l, p, 1], at_y).start()
            remote(r, r, ag_s.at[l, p, 2], ag_r.at[l, p, 2], at_p).start()

    def forward_y(l, *ps):
        for p in ps:
            r = mine(l, p, ix, 1 - y)
            remote(r, r, ag_s.at[l, p, 1], ag_r.at[l, p, 1], at_y).wait_recv()
            remote(r, r, ag_s.at[l, p, 3], ag_r.at[l, p, 3], at_p).start()

    def landed(l, *ps):
        for p in ps:
            for which, half in ((2, y), (3, 1 - y)):
                r = mine(l, p, iq, half)
                remote(r, r, ag_s.at[l, p, which], ag_r.at[l, p, which], at_p).wait_recv()

    def to_peer(l, m):
        src = (wg, wu, wd)[m].at[l]
        dst = (all_g.at[l, rows(RB * i, RB), :], all_u.at[l, rows(RB * i, RB), :], all_d.at[l, rows(C * i, C), :])[m]
        return remote(src, dst, pe_s.at[l, m], pe_r.at[l, m], at_p)

    def from_peer(l):
        for m in range(3):
            to_peer(l, m).wait_recv()

    for l in range(L):
        for p in (0, 1, 2, 3, 8, 4, 5, 6, 7):
            send_x(l, p).start()
        for m in range(3):
            to_peer(l, m).start()

    def stage(l, k, start):
        j, slot = chunk(k), k % 2
        for m, (own, gathered) in enumerate(((wg, all_g), (wu, all_u))):
            for n, (src, row, size) in enumerate(
                (
                    (own.at[l, :, cols(j)], RB * i, RB),
                    (gathered.at[l, rows(RB * ip, RB), cols(j)], RB * ip, RB),
                    (gathered.at[l, rows(2 * RB * (1 - xx), 2 * RB), cols(j)], 2 * RB * (1 - xx), 2 * RB),
                )
            ):
                copy = pltpu.make_async_copy(
                    src, w_gu.at[slot, rows(row, size), m * C : (m + 1) * C], wsem.at[slot, 3 * m + n]
                )
                copy.start() if start else copy.wait()
        theirs = pltpu.make_async_copy(all_d.at[l, rows(C * j, C), :], w_d.at[slot], wsem.at[slot, 6])
        if start:

            @pl.when(j == i)
            def _():
                pltpu.make_async_copy(wd.at[l], w_d.at[slot], wsem.at[slot, 6]).start()

            @pl.when(j != i)
            def _():
                theirs.start()
        else:
            theirs.wait()

    def tile(t):
        return pl.ds(pl.multiple_of(t * TM, TM), TM)

    def clear(ref, size):
        n = ref.shape[0] // size

        @pl.loop(0, n)
        def _(t):
            ref[pl.ds(pl.multiple_of(t * size, size), size), :] = jnp.zeros((size, ref.shape[1]), ref.dtype)

    clear(acc, 256)
    clear(acc_gu, 128)
    clear(acc_d, 128)
    ssq[...] = jnp.zeros_like(ssq)
    load_x.wait()

    @pl.loop(0, T // 256)
    def _(t):
        r = pl.ds(pl.multiple_of(t * 256, 256), 256)
        wide = h[r, :].astype(f32)
        a0[r, :] = (wide * scale_of(wide)).astype(bf16)

    @pl.loop(0, 4)
    def _(k):
        @pl.when(k == 0)
        def _():
            forward_x(0, 0, 1, 2, 3)
            forward_y(0, 0, 1)
            from_peer(0)
            landed(0, 0, 1)

        @pl.when(k == 1)
        def _():
            forward_y(0, 2, 3)
            forward_x(0, 8)
            landed(0, 2, 3)

        @pl.when(k == 2)
        def _():
            forward_x(0, 4, 5, 6, 7)
            forward_y(0, 8)
            landed(0, 8)
            forward_y(0, 4, 5)
            forward_x(1, 0, 1)
            landed(0, 4, 5)

        @pl.when(k == 3)
        def _():
            forward_y(0, 6, 7)
            forward_x(1, 2, 3)
            landed(0, 6, 7)

        stage(0, k, True)
        stage(0, k, False)

        @pl.loop(0, T // TM)
        def _(t):
            r = tile(t)
            gu = dot(a0[r, :], w_gu[k % 2])
            gate, up = gu[:, :C], gu[:, C:]
            act = (gate * jax.nn.sigmoid(gate) * up).astype(bf16)
            acc[r, :] += dot(act, w_d[k % 2])

    forward_y(1, 0, 1)
    from_peer(1)
    landed(1, 0, 1)
    stage(1, 0, True)
    load_dy.wait()

    @pl.loop(0, T // 256)
    def _(t):
        r = pl.ds(pl.multiple_of(t * 256, 256), 256)
        wide = (h[r, :].astype(f32) + acc[r, :].astype(bf16).astype(f32)).astype(bf16)
        h[r, :] = wide
        wide = wide.astype(f32)
        a1[r, :] = (wide * scale_of(wide)).astype(bf16)
        acc[r, :] = jnp.zeros((256, D), f32)

    def d_copies(l, k, act):
        j, s2 = chunk(k), k % 2
        act(remote(sg.at[3], rd3.at[s2], d_s.at[0], d_r3.at[s2], at_p))

        @pl.when(k >= 2)
        def _():
            act(remote(sd.at[rows(DH * (1 - c), DH), :], rd3d.at[s2], d_s.at[1], d_r3d.at[s2], at_p))

        act(remote(sg.at[2], rd2_hbm.at[l, j], d_s.at[2], d_r2.at[l, j], at_p))

        @pl.when((k < 2) & (c != k))
        def _():
            act(remote(sd, rd_d.at[l], d_s.at[3], d_rd.at[l], at_p))

        act(pltpu.make_async_copy(sg.at[0], p0_hbm.at[l, j], keep.at[0]))

        @pl.when((k < 2) & (c == k))
        def _():
            act(pltpu.make_async_copy(sd, own_d.at[l], keep.at[1]))

    def start(copy):
        copy.start()

    def drain(copy):
        copy.wait_send() if copy.is_remote else copy.wait()

    def send_sums(l, k):
        for r, dest in ((3, iq), (1, ix), (2, ip), (0, i)):
            for m in range(2):
                sg[r, RB * m : RB * (m + 1), :] = acc_gu[rows(RB * dest, RB), m * C : (m + 1) * C].astype(bf16)
        sd[...] = acc_d[...].astype(bf16)
        clear(acc_gu, 128)
        clear(acc_d, 128)
        d_copies(l, k, start)

    def x_copy(l, k):
        s4 = k
        return remote(sx.at[s4], rx_hbm.at[l, chunk(k)], x_s.at[s4], x_r.at[l, chunk(k)], at_x)

    def xd_copy(l, k):
        to = (y, 2 * (1 - xx) + k - 2)
        return remote(sxd.at[l, k - 2], rx_d.at[l, rows(DH * c, DH), :], xd_s.at[l, k - 2], xd_r.at[l, c], to)

    def across(l, k, again):
        s2 = k % 2
        remote(sg.at[3], rd3.at[s2], d_s.at[0], d_r3.at[s2], at_p).wait_recv()
        if again:
            x_copy(l, k).wait_send()
        sx[k] = (sg[1].astype(f32) + rd3[s2].astype(f32)).astype(bf16)

        @pl.when(k >= 2)
        def _():
            remote(sd.at[rows(DH * (1 - c), DH), :], rd3d.at[s2], d_s.at[1], d_r3d.at[s2], at_p).wait_recv()
            sxd[l, k - 2] = (sd[rows(DH * c, DH), :].astype(f32) + rd3d[s2].astype(f32)).astype(bf16)

        x_copy(l, k).start()

        @pl.when(k >= 2)
        def _():
            xd_copy(l, k).start()

        d_copies(l, k, drain)

    def add_up(parts, puts):
        for n, part in enumerate(parts):
            pltpu.make_async_copy(part, h.at[n * 384 : (n + 1) * 384, :], fsem.at[n]).start()
        for n, part in enumerate(parts):
            pltpu.make_async_copy(part, h.at[n * 384 : (n + 1) * 384, :], fsem.at[n]).wait()
        for r in range(0, 384, 128):
            g = h[r : r + 128, :].astype(f32) + h[384 + r : 512 + r, :].astype(f32) + h[768 + r : 896 + r, :].astype(f32)
            g = g.astype(bf16)
            h[1152 + r : 1280 + r, :] = g
            g = g.astype(f32)
            ssq[...] += jnp.sum((g * g).reshape(16, 8, D), axis=0)
        outs = []
        for n, (row, size, dst) in enumerate(puts):
            outs.append(pltpu.make_async_copy(h.at[1152 + row : 1152 + row + size, :], dst, fout.at[n]))
        for out in outs:
            out.start()
        for out in outs:
            out.wait()

    def finish_gu(l, k):
        j = chunk_there(k)
        remote(sg.at[2], rd2_hbm.at[l, j], d_s.at[2], d_r2.at[l, j], at_p).wait_recv()
        remote(sx.at[0], rx_hbm.at[l, j], x_s.at[0], x_r.at[l, j], at_x).wait_recv()
        add_up(
            [p0_hbm.at[l, j], rd2_hbm.at[l, j], rx_hbm.at[l, j]],
            [(0, RB, gg_hbm.at[l, :, cols(j)]), (RB, RB, gu_hbm.at[l, :, cols(j)])],
        )

    def finish_d(l):
        remote(sd, rd_d.at[l], d_s.at[3], d_rd.at[l], at_p).wait_recv()
        for half in range(2):
            part = rx_d.at[l, half * DH : (half + 1) * DH, :]
            remote(sxd.at[0, 0], part, xd_s.at[0, 0], xd_r.at[l, half], at_x).wait_recv()
        for half in range(2):
            r = slice(half * DH, (half + 1) * DH)
            add_up([own_d.at[l, r, :], rd_d.at[l, r, :], rx_d.at[l, r, :]], [(0, DH, gd_hbm.at[l, r, :])])

    def backward(l, a, k, t):
        r, slot = tile(t), k % 2
        gu = dot(a[r, :], w_gu[slot])
        dact = dot(do[r, :], w_d[slot], NT).astype(bf16).astype(f32)
        gate, up = gu[:, :C], gu[:, C:]
        sig = jax.nn.sigmoid(gate)
        silu = gate * sig
        act_s[...] = (silu * up).astype(bf16)
        dgu_s[:, C:] = (dact * silu).astype(bf16)
        dgu_s[:, :C] = (dact * up * (sig + silu * (1.0 - sig))).astype(bf16)
        if l:
            acc[r, :] += dot(dgu_s[...], w_gu[slot], NT)
        acc_gu[...] += dot(a[r, :], dgu_s[...], TN)
        acc_d[...] += dot(act_s[...], do[r, :], TN)

    stage(1, 0, False)

    @pl.loop(0, 4)
    def _(k):
        @pl.when(k > 0)
        def _():
            stage(1, k, False)

        @pl.loop(0, T // TM)
        def _(t):
            backward(1, a1, k, t)

            @pl.when((t == 0) & (k > 0))
            def _():
                across(1, k - 1, False)

            @pl.when((t == 1) & (k == 0))
            def _():
                forward_y(1, 2, 3)
                forward_x(1, 8, 4, 5)

            @pl.when((t == 2) & (k == 0))
            def _():
                forward_x(1, 6, 7)
                landed(1, 2, 3)
                stage(1, 1, True)

            @pl.when((t == 1) & (k == 1))
            def _():
                forward_y(1, 8, 4, 5, 6, 7)

            @pl.when((t == 2) & (k == 1))
            def _():
                landed(1, 8, 4, 5)
                stage(1, 2, True)

            @pl.when((t == 2) & (k == 2))
            def _():
                landed(1, 6, 7)
                stage(1, 3, True)

            @pl.when((t == 2) & (k == 3))
            def _():
                stage(0, 0, True)

        send_sums(1, k)

    @pl.loop(0, T // 256)
    def _(t):
        r = pl.ds(pl.multiple_of(t * 256, 256), 256)
        wide = h[r, :].astype(f32)
        scale = scale_of(wide)
        da = acc[r, :].astype(bf16).astype(f32)
        mix = jnp.sum(da * wide, -1, keepdims=True) * (scale * scale * scale / D)
        back = (da * scale - wide * mix).astype(bf16)
        do[r, :] = (do[r, :].astype(f32) + back.astype(f32)).astype(bf16)

    @pl.loop(0, 4)
    def _(k):
        stage(0, k, False)

        @pl.loop(0, T // TM)
        def _(t):
            backward(0, a0, k, t)

            @pl.when((t == 0) & (k == 0))
            def _():
                across(1, 3, False)

            @pl.when((t == 0) & (k > 0))
            def _():
                across(0, k - 1, True)

            @pl.when((t == 2) & (k < 3))
            def _():
                stage(0, k + 1, True)

            @pl.when(t == 2)
            def _():
                finish_gu(1, k)

        send_sums(0, k)

    across(0, 3, True)
    finish_d(1)

    @pl.loop(0, 4)
    def _(k):
        finish_gu(0, k)

    finish_d(0)

    part = ssq[:, :128]
    for n in range(1, D // 128):
        part = part + ssq[:, n * 128 : (n + 1) * 128]
    ss_src[...] = part
    for l in range(L):
        for p in range(9):
            for which, (src, half, to) in enumerate(((ix, y, at_x), (ix, y, at_y), (ix, y, at_p), (ix, 1 - y, at_p))):
                if which == 0:
                    send_x(l, p).wait_send()
                else:
                    r = mine(l, p, src, half)
                    remote(r, r, ag_s.at[l, p, which], ag_r.at[l, p, which], to).wait_send()
        for m in range(3):
            to_peer(l, m).wait_send()
        for k in (2, 3):
            xd_copy(l, k).wait_send()
    for k in range(4):
        x_copy(0, k).wait_send()
    tells = [
        remote(ss_src, ss.at[i], ss_s.at[n], ss_r.at[i], to) for n, to in enumerate((at_x, at_p, at_q))
    ]
    for tell in tells:
        tell.start()
    for src in (ix, ip, iq):
        remote(ss_src, ss.at[src], ss_s.at[0], ss_r.at[src], at_x).wait_recv()
    for tell in tells:
        tell.wait_send()
    ss[i] = part
    total = jnp.sum(ss[0] + ss[1] + ss[2] + ss[3])
    fac[...] = jnp.minimum(1.0, 0.5 * lax.rsqrt(jnp.full((8, 128), total / COUNT + 1e-30, f32)))


def gradients(x, dy, wg, wu, wd):
    hbm = pl.BlockSpec(memory_space=pl.ANY)
    vmem = pl.BlockSpec(memory_space=pltpu.VMEM)
    out = lambda *shape: jax.ShapeDtypeStruct(shape, bf16)
    dma = lambda *shape: pltpu.SemaphoreType.DMA(shape)
    return pl.pallas_call(
        step_kernel,
        in_specs=[hbm] * 5,
        out_specs=[hbm] * 3 + [vmem] + [hbm] * 9,
        out_shape=[
            out(L, RB, FF), out(L, RB, FF), out(L, C, D), jax.ShapeDtypeStruct((8, 128), f32),
            out(L, D, FF), out(L, D, FF), out(L, FF, D),
            out(L, 4, 2 * RB, C), out(L, 4, 2 * RB, C), out(L, 4, 2 * RB, C),
            out(L, C, D), out(L, C, D), out(L, C, D),
        ],
        scratch_shapes=[
            pltpu.VMEM((T, D), bf16), pltpu.VMEM((T, D), bf16), pltpu.VMEM((T, D), bf16), pltpu.VMEM((T, D), bf16),
            pltpu.VMEM((T, D), f32), pltpu.VMEM((D, 2 * C), f32), pltpu.VMEM((C, D), f32),
            pltpu.VMEM((2, D, 2 * C), bf16), pltpu.VMEM((2, C, D), bf16),
            pltpu.VMEM((TM, C), bf16), pltpu.VMEM((TM, 2 * C), bf16),
            pltpu.VMEM((4, 2 * RB, C), bf16), pltpu.VMEM((C, D), bf16),
            pltpu.VMEM((2, 2 * RB, C), bf16), pltpu.VMEM((2, DH, D), bf16),
            pltpu.VMEM((4, 2 * RB, C), bf16), pltpu.VMEM((2, 2, DH, D), bf16),
            pltpu.VMEM((8, D), f32), pltpu.VMEM((4, 8, 128), f32), pltpu.VMEM((8, 128), f32),
            dma(L, 9, 4), dma(L, 9, 4), dma(L, 3), dma(L, 3), dma(2), dma(2, 7),
            dma(4), dma(2), dma(2), dma(L, 4), dma(L), dma(2), dma(4), dma(L, 4), dma(L, 2), dma(L, 2),
            dma(3), dma(2), dma(3), dma(4),
        ],
        compiler_params=pltpu.CompilerParams(
            collective_id=0, has_side_effects=True, vmem_limit_bytes=63 * 2**20
        ),
        name="train_step",
    )(x, dy, wg, wu, wd)


def adamw_kernel(*refs):
    fac, ins, outs = refs[0], refs[1:13], refs[13:]
    factor = fac[0:1, 0:1]
    for n in range(3):
        g, w, m, v = (ins[3 * which + n] for which in range(4))
        grad = g[0].astype(f32) * factor
        new_m = 0.9 * m[0] + 0.1 * grad
        new_v = 0.95 * v[0] + 0.05 * grad * grad
        wide = w[0].astype(f32)
        outs[n][0] = (wide - 0.02 * (new_m * lax.rsqrt(new_v + 1e-8) + 0.1 * wide)).astype(bf16)
        outs[3 + n][0] = new_m
        outs[6 + n][0] = new_v


def adamw(factor, g, w, m, v):
    wide = pl.BlockSpec((1, RB // 12, FF), lambda t: (t // 12, t % 12, 0))
    tall = pl.BlockSpec((1, C // 12, D), lambda t: (t // 12, t % 12, 0))
    specs = [wide, wide, tall]
    shapes = lambda dtype: [jax.ShapeDtypeStruct(a.shape, dtype) for a in w]
    return pl.pallas_call(
        adamw_kernel,
        grid=(24,),
        in_specs=[pl.BlockSpec((8, 128), lambda t: (0, 0))] + specs * 4,
        out_specs=specs * 3,
        out_shape=shapes(bf16) + shapes(f32) + shapes(f32),
        compiler_params=pltpu.CompilerParams(vmem_limit_bytes=63 * 2**20),
        name="adamw",
    )(factor, *g, *w, *m, *v)


def solution(mesh):
    def step(x, dy, *arrays):
        w, m, v = (arrays[n : n + 3] for n in (0, 3, 6))
        gg, gu, gd, factor, *_ = gradients(x[0], dy[0], *w)
        return tuple(adamw(factor, (gg, gu, gd), w, m, v))

    states, cut = P(("rep", "dp"), None, None), P(None, "dp", None)
    return jax.shard_map(
        step,
        mesh=mesh,
        in_specs=(states, states) + (cut,) * 9,
        out_specs=(P("rep", "dp", None),) * 9,
        check_vma=False,
    )
```

```python
import functools

import jax
import jax.numpy as jnp
from jax import lax
from jax.experimental import pallas as pl
from jax.experimental.pallas import tpu as pltpu
from jax.sharding import PartitionSpec as P

T, D, FF, L = 2048, 768, 3072, 2
C = 768
TM = 512
RB = D // 4
RH = RB // 2
DH = C // 2
DQ = C // 4
N = 4
COUNT = 3 * L * D * FF
bf16, f32 = jnp.bfloat16, jnp.float32
NT = (((1,), (1,)), ((), ()))
TN = (((0,), (0,)), ((), ()))
MESH = pl.DeviceIdType.MESH


def dot(a, b, dims=(((1,), (0,)), ((), ()))):
    return lax.dot_general(a, b, dims, preferred_element_type=f32)


def scale_of(wide):
    return lax.rsqrt(jnp.mean(wide * wide, -1, keepdims=True) + 1e-6)


def step_kernel(
    x_hbm, dy_hbm, wg, wu, wd,
    gg_hbm, gu_hbm, gd_hbm, fac, all_g, all_u, all_d, p0_hbm, rd2_hbm, rx_hbm, own_d, rd_d, rx_d,
    h, a0, a1, do, acc, acc_gu, acc_d, w_gu, w_d, act_s, dgu_s, sg, sd, rd3, rd3d, sx, sxd, ssq, ss, ss_src,
    ag_s, ag_r, pe_s, pe_r, ld, wsem, d_s, d_r3, d_r3d, d_r2, d_rd, keep, x_s, x_r, xd_s, xd_r, fsem, fout, ss_s, ss_r,
):
    y, i = lax.axis_index("rep"), lax.axis_index("dp")
    xx, c = i // 2, i % 2
    ix, ip, iq = (1 - xx) * 2 + c, xx * 2 + 1 - c, (1 - xx) * 2 + 1 - c
    at_x, at_p, at_q, at_y = (y, ix), (y, ip), (y, iq), (1 - y, i)

    def remote(src, dst, send, recv, to):
        return pltpu.make_async_remote_copy(
            src_ref=src, dst_ref=dst, send_sem=send, recv_sem=recv, device_id=to, device_id_type=MESH
        )

    def near_first(k):
        return (2 * xx + k) % 4

    def far_first(k):
        return (2 * (1 - xx) + k) % 4

    def start(copy):
        copy.start()

    def drain(copy):
        copy.wait_send() if copy.is_remote else copy.wait()

    def at(t, n, k, m, work):
        pl.when((t == n) & (k == m))(work)

    def cols(j):
        return pl.ds(pl.multiple_of(j * C, C), C)

    def rows(start, size):
        return pl.ds(pl.multiple_of(start, 32), size)

    barrier = pltpu.get_barrier_semaphore()
    for other in (at_x, at_p, at_q, at_y):
        pl.semaphore_signal(barrier, inc=1, device_id=other, device_id_type=MESH)
    load_x = pltpu.make_async_copy(x_hbm, h, ld.at[0])
    load_dy = pltpu.make_async_copy(dy_hbm, do, ld.at[1])
    load_x.start()
    load_dy.start()
    pl.semaphore_wait(barrier, 4)

    def region(l, p, src, half, j):
        if p >= 8:
            return all_d.at[l, rows(C * (src // 2 * 2 + p - 8) + DH * half + DQ * (src % 2), DQ), :]
        return (all_g, all_u)[p % 2].at[l, rows(RB * src + RH * half, RH), cols(j)]

    def mine(l, p, src, half):
        return region(l, p, src, half, (near_first, far_first)[l](p // 2))

    def send_x(l, p, act):
        j = (far_first, near_first)[l](p // 2)
        there = region(l, p, i, y, j)

        def copy(src):
            return remote(src, there, ag_s.at[l, p, 0], ag_r.at[l, p, 0], at_x)

        if p < 8:
            act(copy((wg, wu)[p % 2].at[l, rows(RH * y, RH), cols(j)]))
        elif act is start:

            @pl.when(c == p - 8)
            def _():
                act(copy(wd.at[l, rows(DH * y + DQ * c, DQ), :]))

            @pl.when(c != p - 8)
            def _():
                act(copy(there))
        else:
            act(copy(there))

    def forward_x(l, *ps):
        for p in ps:
            r = mine(l, p, ix, y)
            remote(r, r, ag_s.at[l, p, 0], ag_r.at[l, p, 0], at_x).wait_recv()
            remote(r, r, ag_s.at[l, p, 1], ag_r.at[l, p, 1], at_y).start()
            remote(r, r, ag_s.at[l, p, 2], ag_r.at[l, p, 2], at_p).start()

    def forward_y(l, *ps):
        for p in ps:
            r = mine(l, p, ix, 1 - y)
            remote(r, r, ag_s.at[l, p, 1], ag_r.at[l, p, 1], at_y).wait_recv()
            remote(r, r, ag_s.at[l, p, 3], ag_r.at[l, p, 3], at_p).start()

    def landed(l, *ps):
        for p in ps:
            for which, half in ((2, y), (3, 1 - y)):
                r = mine(l, p, iq, half)
                remote(r, r, ag_s.at[l, p, which], ag_r.at[l, p, which], at_p).wait_recv()

    def to_peer(l, m):
        src = (wg, wu, wd)[m].at[l]
        dst = (all_g.at[l, rows(RB * i, RB), :], all_u.at[l, rows(RB * i, RB), :], all_d.at[l, rows(C * i, C), :])[m]
        return remote(src, dst, pe_s.at[l, m], pe_r.at[l, m], at_p)

    def from_peer(l):
        for m in range(3):
            to_peer(l, m).wait_recv()

    for p in range(6):
        send_x(0, p, start)
    for l in range(L):
        for m in range(3):
            to_peer(l, m).start()

    def stage_gu(l, k, j, act):
        slot = k % 2
        for m, (own, gathered) in enumerate(((wg, all_g), (wu, all_u))):
            for n, (src, row, size) in enumerate(
                (
                    (own.at[l, :, cols(j)], RB * i, RB),
                    (gathered.at[l, rows(RB * ip, RB), cols(j)], RB * ip, RB),
                    (gathered.at[l, rows(2 * RB * (1 - xx), 2 * RB), cols(j)], 2 * RB * (1 - xx), 2 * RB),
                )
            ):
                copy = pltpu.make_async_copy(
                    src, w_gu.at[slot, rows(row, size), m * C : (m + 1) * C], wsem.at[slot, 3 * m + n]
                )
                act(copy)

    def stage_d(l, k, j, act):
        slot = k % 2
        theirs = pltpu.make_async_copy(all_d.at[l, rows(C * j, C), :], w_d.at[slot], wsem.at[slot, 6])
        if act is start:

            @pl.when(j == i)
            def _():
                pltpu.make_async_copy(wd.at[l], w_d.at[slot], wsem.at[slot, 6]).start()

            @pl.when(j != i)
            def _():
                theirs.start()
        else:
            act(theirs)

    def stage(l, k, j, act):
        stage_gu(l, k, j, act)
        stage_d(l, k, j, act)

    def tile(t):
        return pl.ds(pl.multiple_of(t * TM, TM), TM)

    def clear(ref, size):
        n = ref.shape[0] // size

        @pl.loop(0, n)
        def _(t):
            ref[pl.ds(pl.multiple_of(t * size, size), size), :] = jnp.zeros((size, ref.shape[1]), ref.dtype)

    clear(acc, 256)
    clear(acc_gu, 128)
    clear(acc_d, 128)
    ssq[...] = jnp.zeros_like(ssq)
    load_x.wait()

    @pl.loop(0, T // 256)
    def _(t):
        r = pl.ds(pl.multiple_of(t * 256, 256), 256)
        wide = h[r, :].astype(f32)
        a0[r, :] = (wide * scale_of(wide)).astype(bf16)

    def forward(k, t):
        r = tile(t)
        gu = dot(a0[r, :], w_gu[k % 2])
        gate, up = gu[:, :C], gu[:, C:]
        act = (gate * jax.nn.sigmoid(gate) * up).astype(bf16)
        acc[r, :] += dot(act, w_d[k % 2])

    forward_x(0, 0, 1)
    from_peer(0)
    for p in (8, 6, 7, 9):
        send_x(0, p, start)
    forward_x(0, 2, 3)
    forward_y(0, 0, 1)
    landed(0, 0, 1)
    stage(0, 0, near_first(0), start)

    @pl.loop(0, 4)
    def _(k):
        stage(0, k, near_first(k), drain)

        @pl.loop(0, T // TM)
        def _(t):
            forward(k, t)

            @functools.partial(at, t, 0, k, 0)
            def _():
                forward_y(0, 2, 3)
                forward_x(0, 4, 5)

            @functools.partial(at, t, 1, k, 0)
            def _():
                from_peer(1)
                for p in (0, 1, 8, 2, 3, 9, 4, 5, 6, 7):
                    send_x(1, p, start)

            @functools.partial(at, t, 2, k, 0)
            def _():
                landed(0, 2, 3)
                stage(0, 1, near_first(1), start)

            @functools.partial(at, t, 3, k, 0)
            def _():
                forward_x(0, 8)
                forward_y(0, 4, 5)

            @functools.partial(at, t, 1, k, 1)
            def _():
                landed(0, 4, 5)
                stage_gu(0, 2, near_first(2), start)

            @functools.partial(at, t, 2, k, 1)
            def _():
                forward_x(0, 6, 7)
                forward_y(0, 8)

            @functools.partial(at, t, 3, k, 1)
            def _():
                landed(0, 8)
                stage_d(0, 2, near_first(2), start)

            @functools.partial(at, t, 0, k, 2)
            def _():
                forward_x(0, 9)
                forward_y(0, 6, 7)

            @functools.partial(at, t, 2, k, 2)
            def _():
                landed(0, 6, 7)
                stage_gu(0, 3, near_first(3), start)

            @functools.partial(at, t, 3, k, 2)
            def _():
                forward_y(0, 9)
                forward_x(1, 0, 1)
                landed(0, 9)
                stage_d(0, 3, near_first(3), start)

            @functools.partial(at, t, 1, k, 3)
            def _():
                forward_y(1, 0, 1)
                forward_x(1, 8)

            @functools.partial(at, t, 3, k, 3)
            def _():
                forward_y(1, 8)
                forward_x(1, 2, 3)
                landed(1, 0, 1)
                stage_gu(1, 0, far_first(0), start)
                landed(1, 8)
                stage_d(1, 0, far_first(0), start)

    load_dy.wait()

    @pl.loop(0, T // 256)
    def _(t):
        r = pl.ds(pl.multiple_of(t * 256, 256), 256)
        wide = (h[r, :].astype(f32) + acc[r, :].astype(bf16).astype(f32)).astype(bf16)
        h[r, :] = wide
        wide = wide.astype(f32)
        a1[r, :] = (wide * scale_of(wide)).astype(bf16)
        acc[r, :] = jnp.zeros((256, D), f32)

    def d_copies(l, k, act):
        j, s2 = far_first(k), k % 2
        act(remote(sg.at[3], rd3.at[s2], d_s.at[0], d_r3.at[s2], at_p))

        @pl.when(k < 2)
        def _():
            act(remote(sd.at[rows(DH * (1 - c), DH), :], rd3d.at[s2], d_s.at[1], d_r3d.at[s2], at_p))

        act(remote(sg.at[2], rd2_hbm.at[l, j], d_s.at[2], d_r2.at[l, j], at_p))

        @pl.when((k >= 2) & (c != k - 2))
        def _():
            act(remote(sd, rd_d.at[l], d_s.at[3], d_rd.at[l], at_p))

        act(pltpu.make_async_copy(sg.at[0], p0_hbm.at[l, j], keep.at[0]))

        @pl.when((k >= 2) & (c == k - 2))
        def _():
            act(pltpu.make_async_copy(sd, own_d.at[l], keep.at[1]))

    def send_sums(l, k):
        for r, dest in ((3, iq), (1, ix), (2, ip), (0, i)):
            for m in range(2):
                sg[r, RB * m : RB * (m + 1), :] = acc_gu[rows(RB * dest, RB), m * C : (m + 1) * C].astype(bf16)
        sd[...] = acc_d[...].astype(bf16)
        clear(acc_gu, 128)
        clear(acc_d, 128)
        d_copies(l, k, start)

    def x_copy(l, k):
        j = far_first(k)
        return remote(sx.at[k], rx_hbm.at[l, j], x_s.at[k], x_r.at[l, j], at_x)

    def xd_copy(l, k):
        to = (y, 2 * (1 - xx) + k)
        return remote(sxd.at[l, k], rx_d.at[l, rows(DH * c, DH), :], xd_s.at[l, k], xd_r.at[l, c], to)

    def across(l, k, again):
        s2 = k % 2
        remote(sg.at[3], rd3.at[s2], d_s.at[0], d_r3.at[s2], at_p).wait_recv()
        if again:
            x_copy(l, k).wait_send()
        sx[k] = (sg[1].astype(f32) + rd3[s2].astype(f32)).astype(bf16)

        @pl.when(k < 2)
        def _():
            remote(sd.at[rows(DH * (1 - c), DH), :], rd3d.at[s2], d_s.at[1], d_r3d.at[s2], at_p).wait_recv()
            sxd[l, k] = (sd[rows(DH * c, DH), :].astype(f32) + rd3d[s2].astype(f32)).astype(bf16)

        x_copy(l, k).start()

        @pl.when(k < 2)
        def _():
            xd_copy(l, k).start()

        d_copies(l, k, drain)

    def bring(n, part, act):
        act(pltpu.make_async_copy(part, h.at[n * 384 : (n + 1) * 384, :], fsem.at[n]))

    def put(n, dst, act):
        act(pltpu.make_async_copy(h.at[1152 + RB * n : 1152 + RB * (n + 1), :], dst, fout.at[n]))

    def add_up(parts, puts):
        for n, part in enumerate(parts):
            bring(n, part, drain)
        for r in range(0, 384, 128):
            g = h[r : r + 128, :].astype(f32) + h[384 + r : 512 + r, :].astype(f32) + h[768 + r : 896 + r, :].astype(f32)
            g = g.astype(bf16)
            h[1152 + r : 1280 + r, :] = g
            g = g.astype(f32)
            ssq[...] += jnp.sum((g * g).reshape(16, 8, D), axis=0)
        for n, dst in enumerate(puts):
            put(n, dst, start)

    def put_done():
        for n in range(2):
            put(n, gg_hbm.at[0, :, 0:C], drain)

    def gu_parts(l, k):
        j = near_first(k)
        return [p0_hbm.at[l, j], rd2_hbm.at[l, j], rx_hbm.at[l, j]]

    def bring_gu(l, k):
        j = near_first(k)
        parts = gu_parts(l, k)
        remote(sg.at[2], parts[1], d_s.at[2], d_r2.at[l, j], at_p).wait_recv()
        bring(0, parts[0], start)
        bring(1, parts[1], start)
        remote(sx.at[0], parts[2], x_s.at[0], x_r.at[l, j], at_x).wait_recv()
        bring(2, parts[2], start)

    def add_gu(l, k):
        j = near_first(k)
        add_up(gu_parts(l, k), [gg_hbm.at[l, :, cols(j)], gu_hbm.at[l, :, cols(j)]])

    def d_parts(l, half):
        r = rows(half * DH, DH)
        return [own_d.at[l, r, :], rd_d.at[l, r, :], rx_d.at[l, r, :]]

    def bring_d(l, half):
        parts = d_parts(l, half)
        remote(sxd.at[0, 0], parts[2], xd_s.at[0, 0], xd_r.at[l, half], at_x).wait_recv()
        for n, part in enumerate(parts):
            bring(n, part, start)

    def add_d(l, half):
        add_up(d_parts(l, half), [gd_hbm.at[l, rows(half * DH + RB * n, RB), :] for n in range(2)])

    def other_core_d(l):
        remote(sd, rd_d.at[l], d_s.at[3], d_rd.at[l], at_p).wait_recv()

    def backward(l, a, k, t):
        r, slot = tile(t), k % 2
        gu = dot(a[r, :], w_gu[slot])
        dact = dot(do[r, :], w_d[slot], NT).astype(bf16).astype(f32)
        gate, up = gu[:, :C], gu[:, C:]
        sig = jax.nn.sigmoid(gate)
        silu = gate * sig
        act_s[...] = (silu * up).astype(bf16)
        dgu_s[:, C:] = (dact * silu).astype(bf16)
        dgu_s[:, :C] = (dact * up * (sig + silu * (1.0 - sig))).astype(bf16)
        if l:
            acc[r, :] += dot(dgu_s[...], w_gu[slot], NT)
        acc_gu[...] += dot(a[r, :], dgu_s[...], TN)
        acc_d[...] += dot(act_s[...], do[r, :], TN)

    @pl.loop(0, 4)
    def _(k):
        stage(1, k, far_first(k), drain)

        @pl.loop(0, T // TM)
        def _(t):
            backward(1, a1, k, t)

            @pl.when((t == 0) & (k > 0))
            def _():
                across(1, k - 1, False)

            @functools.partial(at, t, 0, k, 0)
            def _():
                forward_y(1, 2, 3)
                forward_x(1, 9)

            @functools.partial(at, t, 1, k, 0)
            def _():
                forward_y(1, 9)
                forward_x(1, 4, 5)

            @functools.partial(at, t, 2, k, 0)
            def _():
                forward_y(1, 4, 5)
                forward_x(1, 6, 7)
                landed(1, 2, 3, 9)
                stage(1, 1, far_first(1), start)

            @functools.partial(at, t, 0, k, 1)
            def _():
                forward_y(1, 6, 7)

            @functools.partial(at, t, 2, k, 1)
            def _():
                landed(1, 4, 5)
                stage(1, 2, far_first(2), start)

            @functools.partial(at, t, 2, k, 2)
            def _():
                landed(1, 6, 7)
                stage(1, 3, far_first(3), start)

            @functools.partial(at, t, 2, k, 3)
            def _():
                stage(0, 0, far_first(0), start)

        send_sums(1, k)

    @pl.loop(0, T // 256)
    def _(t):
        r = pl.ds(pl.multiple_of(t * 256, 256), 256)
        wide = h[r, :].astype(f32)
        scale = scale_of(wide)
        da = acc[r, :].astype(bf16).astype(f32)
        mix = jnp.sum(da * wide, -1, keepdims=True) * (scale * scale * scale / D)
        back = (da * scale - wide * mix).astype(bf16)
        do[r, :] = (do[r, :].astype(f32) + back.astype(f32)).astype(bf16)

    @pl.loop(0, 4)
    def _(k):
        stage(0, k, far_first(k), drain)

        @pl.loop(0, T // TM)
        def _(t):
            backward(0, a0, k, t)

            @pl.when((t == 0) & (k == 0))
            def _():
                across(1, 3, False)

            @pl.when((t == 0) & (k > 0))
            def _():
                across(0, k - 1, True)
                put_done()

            @pl.when(t == 0)
            def _():
                bring_gu(1, k)

            @pl.when(t == 1)
            def _():
                add_gu(1, k)

            @pl.when((t == 2) & (k < 3))
            def _():
                stage(0, k + 1, far_first(k + 1), start)

            @functools.partial(at, t, 2, k, 0)
            def _():
                other_core_d(1)

            @pl.when((t == 2) & (k < 2))
            def _():
                put_done()
                bring_d(1, k)

            @pl.when((t == 3) & (k < 2))
            def _():
                add_d(1, k)

        send_sums(0, k)

    across(0, 3, True)
    other_core_d(0)

    @pl.loop(0, 2)
    def _(k):
        put_done()
        bring_gu(0, k)
        add_gu(0, k)
        put_done()
        bring_d(0, k)
        add_d(0, k)

    @pl.loop(2, 4)
    def _(k):
        put_done()
        bring_gu(0, k)
        add_gu(0, k)

    part = ssq[:, :128]
    for n in range(1, D // 128):
        part = part + ssq[:, n * 128 : (n + 1) * 128]
    ss_src[...] = part
    for l in range(L):
        for p in range(10):
            for which, (src, half, to) in enumerate(((ix, y, at_x), (ix, y, at_y), (ix, y, at_p), (ix, 1 - y, at_p))):
                if which == 0:
                    send_x(l, p, drain)
                else:
                    r = mine(l, p, src, half)
                    remote(r, r, ag_s.at[l, p, which], ag_r.at[l, p, which], to).wait_send()
        for m in range(3):
            to_peer(l, m).wait_send()
        for k in (0, 1):
            xd_copy(l, k).wait_send()
    for k in range(4):
        x_copy(0, k).wait_send()
    tells = [
        remote(ss_src, ss.at[i], ss_s.at[n], ss_r.at[i], to) for n, to in enumerate((at_x, at_p, at_q))
    ]
    for tell in tells:
        tell.start()
    for src in (ix, ip, iq):
        remote(ss_src, ss.at[src], ss_s.at[0], ss_r.at[src], at_x).wait_recv()
    for tell in tells:
        tell.wait_send()
    put_done()
    ss[i] = part
    total = jnp.sum(ss[0] + ss[1] + ss[2] + ss[3])
    fac[...] = jnp.minimum(1.0, 0.5 * lax.rsqrt(jnp.full((8, 128), total / COUNT + 1e-30, f32)))


def gradients(x, dy, wg, wu, wd):
    hbm = pl.BlockSpec(memory_space=pl.ANY)
    vmem = pl.BlockSpec(memory_space=pltpu.VMEM)
    out = lambda *shape: jax.ShapeDtypeStruct(shape, bf16)
    dma = lambda *shape: pltpu.SemaphoreType.DMA(shape)
    return pl.pallas_call(
        step_kernel,
        in_specs=[hbm] * 5,
        out_specs=[hbm] * 3 + [vmem] + [hbm] * 9,
        out_shape=[
            out(L, RB, FF), out(L, RB, FF), out(L, C, D), jax.ShapeDtypeStruct((8, 128), f32),
            out(L, D, FF), out(L, D, FF), out(L, FF, D),
            out(L, 4, 2 * RB, C), out(L, 4, 2 * RB, C), out(L, 4, 2 * RB, C),
            out(L, C, D), out(L, C, D), out(L, C, D),
        ],
        scratch_shapes=[
            pltpu.VMEM((T, D), bf16), pltpu.VMEM((T, D), bf16), pltpu.VMEM((T, D), bf16), pltpu.VMEM((T, D), bf16),
            pltpu.VMEM((T, D), f32), pltpu.VMEM((D, 2 * C), f32), pltpu.VMEM((C, D), f32),
            pltpu.VMEM((2, D, 2 * C), bf16), pltpu.VMEM((2, C, D), bf16),
            pltpu.VMEM((TM, C), bf16), pltpu.VMEM((TM, 2 * C), bf16),
            pltpu.VMEM((4, 2 * RB, C), bf16), pltpu.VMEM((C, D), bf16),
            pltpu.VMEM((2, 2 * RB, C), bf16), pltpu.VMEM((2, DH, D), bf16),
            pltpu.VMEM((4, 2 * RB, C), bf16), pltpu.VMEM((2, 2, DH, D), bf16),
            pltpu.VMEM((8, D), f32), pltpu.VMEM((4, 8, 128), f32), pltpu.VMEM((8, 128), f32),
            dma(L, 10, 4), dma(L, 10, 4), dma(L, 3), dma(L, 3), dma(2), dma(2, 7),
            dma(4), dma(2), dma(2), dma(L, 4), dma(L), dma(2), dma(4), dma(L, 4), dma(L, 2), dma(L, 2),
            dma(3), dma(2), dma(3), dma(4),
        ],
        compiler_params=pltpu.CompilerParams(
            collective_id=0, has_side_effects=True, vmem_limit_bytes=63 * 2**20
        ),
        name="train_step",
    )(x, dy, wg, wu, wd)


def adamw_kernel(*refs):
    fac, ins, outs = refs[0], refs[1:13], refs[13:]
    factor = fac[0:1, 0:1]
    for n in range(3):
        g, w, m, v = (ins[3 * which + n] for which in range(4))
        grad = g[0].astype(f32) * factor
        new_m = 0.9 * m[0] + 0.1 * grad
        new_v = 0.95 * v[0] + 0.05 * grad * grad
        wide = w[0].astype(f32)
        outs[n][0] = (wide - 0.02 * (new_m * lax.rsqrt(new_v + 1e-8) + 0.1 * wide)).astype(bf16)
        outs[3 + n][0] = new_m
        outs[6 + n][0] = new_v


def adamw(factor, g, w, m, v):
    wide = pl.BlockSpec((1, RB // N, FF), lambda t: (t // N, t % N, 0))
    tall = pl.BlockSpec((1, C // N, D), lambda t: (t // N, t % N, 0))
    specs = [wide, wide, tall]
    shapes = lambda dtype: [jax.ShapeDtypeStruct(a.shape, dtype) for a in w]
    return pl.pallas_call(
        adamw_kernel,
        grid=(L * N,),
        in_specs=[pl.BlockSpec((8, 128), lambda t: (0, 0))] + specs * 4,
        out_specs=specs * 3,
        out_shape=shapes(bf16) + shapes(f32) + shapes(f32),
        compiler_params=pltpu.CompilerParams(vmem_limit_bytes=63 * 2**20),
        name="adamw",
    )(factor, *g, *w, *m, *v)


def solution(mesh):
    def step(x, dy, *arrays):
        w, m, v = (arrays[n : n + 3] for n in (0, 3, 6))
        gg, gu, gd, factor, *_ = gradients(x[0], dy[0], *w)
        return tuple(adamw(factor, (gg, gu, gd), w, m, v))

    states, cut = P(("rep", "dp"), None, None), P(None, "dp", None)
    return jax.shard_map(
        step,
        mesh=mesh,
        in_specs=(states, states) + (cut,) * 9,
        out_specs=(P("rep", "dp", None),) * 9,
        check_vma=False,
    )
```

```python
import functools

import jax
import jax.numpy as jnp
from jax import lax
from jax.experimental import pallas as pl
from jax.experimental.pallas import tpu as pltpu
from jax.sharding import PartitionSpec as P

T, D, FF, L = 2048, 768, 3072, 2
C = 768
TM = 512
RB = D // 4
RH = RB // 2
DH = C // 2
DQ = C // 4
N = 4
COUNT = 3 * L * D * FF
FIRST, SECOND, THIRD, LAST = range(4)
OVER_X, OVER_Y, TO_CORE, Y_TO_CORE = range(4)
GU = [(n, n + 1) for n in range(0, 8, 2)]
GU_1, GU_2, GU_3, GU_4 = GU
DOWN_1, DOWN_2 = (8,), (9,)
ONE, TWO = range(L)
bf16, f32 = jnp.bfloat16, jnp.float32
NT = (((1,), (1,)), ((), ()))
TN = (((0,), (0,)), ((), ()))
MESH = pl.DeviceIdType.MESH


def dot(a, b, dims=(((1,), (0,)), ((), ()))):
    return lax.dot_general(a, b, dims, preferred_element_type=f32)


def scale_of(wide):
    return lax.rsqrt(jnp.mean(wide * wide, -1, keepdims=True) + 1e-6)


def step_kernel(
    x_hbm, dy_hbm, wg, wu, wd,
    gg_hbm, gu_hbm, gd_hbm, fac, all_g, all_u, all_d, p0_hbm, rd2_hbm, rx_hbm, own_d, rd_d, rx_d, up_hbm, act_hbm,
    h, a0, a1, do, acc, acc_gu, acc_d, w_gu, w_d, act_s, dgu_s, sg, sd, rd3, rd3d, sx, sxd, ssq, ss, ss_src, up_s,
    ag_s, ag_r, pe_s, pe_r, ld, wsem, d_s, d_r3, dd_s, d_r3d, d_r2, d_rd, keep, x_s, x_r, xd_s, xd_r, fsem, fout, ss_s, ss_r, save, back,
):
    y, i = lax.axis_index("rep"), lax.axis_index("dp")
    xx, c = i // 2, i % 2
    ix, ip, iq = (1 - xx) * 2 + c, xx * 2 + 1 - c, (1 - xx) * 2 + 1 - c
    at_x, at_p, at_q, at_y = (y, ix), (y, ip), (y, iq), (1 - y, i)

    def remote(src, dst, send, recv, to):
        return pltpu.make_async_remote_copy(
            src_ref=src, dst_ref=dst, send_sem=send, recv_sem=recv, device_id=to, device_id_type=MESH
        )

    def near_first(k):
        return (2 * xx + k) % 4

    def far_first(k):
        return (2 * (1 - xx) + k) % 4

    def far_between(k, side=xx):
        return 2 * ((side + (k + 1) // 2) % 2) + k // 2

    def start(copy):
        copy.start()

    def drain(copy):
        copy.wait_send() if copy.is_remote else copy.wait()

    def at(t, n, k, m):
        return pl.when((t == n) & (k == m))

    def cols(j):
        return pl.ds(pl.multiple_of(j * C, C), C)

    def rows(start, size):
        return pl.ds(pl.multiple_of(start, 32), size)

    barrier = pltpu.get_barrier_semaphore()
    for other in (at_x, at_p, at_q, at_y):
        pl.semaphore_signal(barrier, inc=1, device_id=other, device_id_type=MESH)
    load_x = pltpu.make_async_copy(x_hbm, h, ld.at[0])
    load_dy = pltpu.make_async_copy(dy_hbm, do, ld.at[1])
    load_x.start()
    load_dy.start()
    pl.semaphore_wait(barrier, 4)

    def region(l, p, src, half, j):
        if p >= 8:
            return all_d.at[l, rows(C * (src // 2 * 2 + p - 8) + DH * half + DQ * (src % 2), DQ), :]
        return (all_g, all_u)[p % 2].at[l, rows(RB * src + RH * half, RH), cols(j)]

    def mine(l, p, src, half):
        return region(l, p, src, half, (near_first, far_between)[l](p // 2))

    def send_x(l, p, act):
        j = far_between(p // 2, 1 - xx) if l else far_first(p // 2)
        there = region(l, p, i, y, j)

        def copy(src):
            return remote(src, there, ag_s.at[l, p, OVER_X], ag_r.at[l, p, OVER_X], at_x)

        if p < 8:
            act(copy((wg, wu)[p % 2].at[l, rows(RH * y, RH), cols(j)]))
        elif act is start:

            @pl.when(c == p - 8)
            def _():
                act(copy(wd.at[l, rows(DH * y + DQ * c, DQ), :]))

            @pl.when(c != p - 8)
            def _():
                act(copy(there))
        else:
            act(copy(there))

    def forward_x(l, *pieces):
        for p in sum(pieces, ()):
            r = mine(l, p, ix, y)
            remote(r, r, ag_s.at[l, p, OVER_X], ag_r.at[l, p, OVER_X], at_x).wait_recv()
            remote(r, r, ag_s.at[l, p, OVER_Y], ag_r.at[l, p, OVER_Y], at_y).start()
            remote(r, r, ag_s.at[l, p, TO_CORE], ag_r.at[l, p, TO_CORE], at_p).start()

    def forward_y(l, *pieces):
        for p in sum(pieces, ()):
            r = mine(l, p, ix, 1 - y)
            remote(r, r, ag_s.at[l, p, OVER_Y], ag_r.at[l, p, OVER_Y], at_y).wait_recv()
            remote(r, r, ag_s.at[l, p, Y_TO_CORE], ag_r.at[l, p, Y_TO_CORE], at_p).start()

    def landed(l, *pieces):
        for p in sum(pieces, ()):
            for which, half in ((TO_CORE, y), (Y_TO_CORE, 1 - y)):
                r = mine(l, p, iq, half)
                remote(r, r, ag_s.at[l, p, which], ag_r.at[l, p, which], at_p).wait_recv()

    def to_peer(l, m):
        src = (wg, wu, wd)[m].at[l]
        dst = (all_g.at[l, rows(RB * i, RB), :], all_u.at[l, rows(RB * i, RB), :], all_d.at[l, rows(C * i, C), :])[m]
        return remote(src, dst, pe_s.at[l, m], pe_r.at[l, m], at_p)

    def from_peer(l):
        for m in range(3):
            to_peer(l, m).wait_recv()

    def send(l, *pieces):
        for p in sum(pieces, ()):
            send_x(l, p, start)

    send(ONE, GU_1, GU_2, GU_3)
    for l in range(L):
        for m in range(3):
            to_peer(l, m).start()

    def stage_gu(l, k, j, act):
        slot = k % 2
        for m, (own, gathered) in enumerate(((wg, all_g), (wu, all_u))):
            for n, (src, row, size) in enumerate(
                (
                    (own.at[l, :, cols(j)], RB * i, RB),
                    (gathered.at[l, rows(RB * ip, RB), cols(j)], RB * ip, RB),
                    (gathered.at[l, rows(2 * RB * (1 - xx), 2 * RB), cols(j)], 2 * RB * (1 - xx), 2 * RB),
                )
            ):
                copy = pltpu.make_async_copy(
                    src, w_gu.at[slot, rows(row, size), m * C : (m + 1) * C], wsem.at[slot, 3 * m + n]
                )
                act(copy)

    def stage_d(l, k, j, act):
        slot = k % 2
        theirs = pltpu.make_async_copy(all_d.at[l, rows(C * j, C), :], w_d.at[slot], wsem.at[slot, 6])
        if act is start:

            @pl.when(j == i)
            def _():
                pltpu.make_async_copy(wd.at[l], w_d.at[slot], wsem.at[slot, 6]).start()

            @pl.when(j != i)
            def _():
                theirs.start()
        else:
            act(theirs)

    def stage(l, k, j, act):
        stage_gu(l, k, j, act)
        stage_d(l, k, j, act)

    def tile(t):
        return pl.ds(pl.multiple_of(t * TM, TM), TM)

    def clear(ref, size):
        n = ref.shape[0] // size

        @pl.loop(0, n)
        def _(t):
            ref[pl.ds(pl.multiple_of(t * size, size), size), :] = jnp.zeros((size, ref.shape[1]), ref.dtype)

    clear(acc, 256)
    clear(acc_gu, 128)
    clear(acc_d, 128)
    ssq[...] = jnp.zeros_like(ssq)
    load_x.wait()

    @pl.loop(0, T // 256)
    def _(t):
        r = pl.ds(pl.multiple_of(t * 256, 256), 256)
        wide = h[r, :].astype(f32)
        a0[r, :] = (wide * scale_of(wide)).astype(bf16)

    def saving(j, t, act):
        s = t % 2
        act(pltpu.make_async_copy(up_s.at[s], up_hbm.at[j, tile(t), :], save.at[0, s]))
        act(pltpu.make_async_copy(dgu_s.at[:, cols(s)], act_hbm.at[j, tile(t), :], save.at[1, s]))

    def forward(k, t):
        r, s = tile(t), t % 2

        @pl.when((k > 0) | (t > 1))
        def _():
            saving(near_first(k), t, drain)

        gu = dot(a0[r, :], w_gu[k % 2])
        up_s[s] = gu
        gate, up = gu[:, :C], gu[:, C:]
        act = (gate * jax.nn.sigmoid(gate) * up).astype(bf16)
        dgu_s[:, cols(s)] = act
        saving(near_first(k), t, start)
        acc[r, :] += dot(act, w_d[k % 2])

    forward_x(ONE, GU_1)
    from_peer(ONE)
    send(ONE, DOWN_1, GU_4, DOWN_2)
    forward_x(ONE, GU_2)
    forward_y(ONE, GU_1)
    landed(ONE, GU_1)
    stage(ONE, FIRST, near_first(FIRST), start)

    @pl.loop(0, 4)
    def _(k):
        stage(ONE, k, near_first(k), drain)

        @pl.loop(0, T // TM)
        def _(t):
            forward(k, t)

            @at(t, FIRST, k, FIRST)
            def _():
                forward_y(ONE, GU_2)
                forward_x(ONE, GU_3)

            @at(t, SECOND, k, FIRST)
            def _():
                from_peer(TWO)
                send(TWO, GU_1, GU_2, DOWN_1, GU_3, DOWN_2, GU_4)

            @at(t, THIRD, k, FIRST)
            def _():
                landed(ONE, GU_2)
                stage(ONE, SECOND, near_first(SECOND), start)

            @at(t, LAST, k, FIRST)
            def _():
                forward_x(ONE, DOWN_1)
                forward_y(ONE, GU_3)

            @at(t, SECOND, k, SECOND)
            def _():
                landed(ONE, GU_3)
                stage_gu(ONE, THIRD, near_first(THIRD), start)

            @at(t, THIRD, k, SECOND)
            def _():
                forward_x(ONE, GU_4)
                forward_y(ONE, DOWN_1)

            @at(t, LAST, k, SECOND)
            def _():
                landed(ONE, DOWN_1)
                stage_d(ONE, THIRD, near_first(THIRD), start)

            @at(t, FIRST, k, THIRD)
            def _():
                forward_x(ONE, DOWN_2)
                forward_y(ONE, GU_4)

            @at(t, THIRD, k, THIRD)
            def _():
                landed(ONE, GU_4)
                stage_gu(ONE, LAST, near_first(LAST), start)
                forward_x(TWO, GU_1)

            @at(t, LAST, k, THIRD)
            def _():
                forward_y(ONE, DOWN_2)
                landed(ONE, DOWN_2)
                stage_d(ONE, LAST, near_first(LAST), start)

            @at(t, FIRST, k, LAST)
            def _():
                forward_x(TWO, GU_2)
                forward_y(TWO, GU_1)

            @at(t, THIRD, k, LAST)
            def _():
                forward_x(TWO, DOWN_1)
                forward_y(TWO, GU_2)
                landed(TWO, GU_1)
                stage(TWO, FIRST, far_between(FIRST), start)

    for n in (THIRD, LAST):
        saving(near_first(LAST), n, drain)
    load_dy.wait()

    @pl.loop(0, T // 256)
    def _(t):
        r = pl.ds(pl.multiple_of(t * 256, 256), 256)
        wide = (h[r, :].astype(f32) + acc[r, :].astype(bf16).astype(f32)).astype(bf16)
        h[r, :] = wide
        wide = wide.astype(f32)
        a1[r, :] = (wide * scale_of(wide)).astype(bf16)
        acc[r, :] = jnp.zeros((256, D), f32)

    def gu_copies(l, k, j, act):
        act(remote(sg.at[3], rd3.at[k % 2], d_s.at[0], d_r3.at[k % 2], at_p))
        act(remote(sg.at[2], rd2_hbm.at[l, j], d_s.at[1], d_r2.at[l, j], at_p))
        act(pltpu.make_async_copy(sg.at[0], p0_hbm.at[l, j], keep.at[0]))

    def far_copy(q):
        return remote(sd.at[q, rows(DH * (1 - c), DH), :], rd3d.at[q], dd_s.at[0, q], d_r3d.at[q], at_p)

    def near_copy(l, q, act):
        @pl.when(c != q)
        def _():
            act(remote(sd.at[q], rd_d.at[l], dd_s.at[1, q], d_rd.at[l], at_p))

        @pl.when(c == q)
        def _():
            act(pltpu.make_async_copy(sd.at[q], own_d.at[l], keep.at[1]))

    def round_gu():
        for r, dest in ((3, iq), (1, ix), (2, ip), (0, i)):
            for m in range(2):
                sg[r, RB * m : RB * (m + 1), :] = acc_gu[rows(RB * dest, RB), m * C : (m + 1) * C].astype(bf16)
        clear(acc_gu, 128)

    def round_d(q):
        sd[q] = acc_d[...].astype(bf16)
        clear(acc_d, 128)

    def x_copy(l, k, j):
        return remote(sx.at[k], rx_hbm.at[l, j], x_s.at[k], x_r.at[l, j], at_x)

    def xd_copy(l, q):
        return remote(sxd.at[l, q], rx_d.at[l, rows(DH * c, DH), :], xd_s.at[l, q], xd_r.at[l, c], (y, 2 * (1 - xx) + q))

    def gu_across(l, k, j):
        remote(sg.at[3], rd3.at[k % 2], d_s.at[0], d_r3.at[k % 2], at_p).wait_recv()
        if l == ONE:
            x_copy(l, k, j).wait_send()
        sx[k] = (sg[1].astype(f32) + rd3[k % 2].astype(f32)).astype(bf16)
        x_copy(l, k, j).start()
        gu_copies(l, k, j, drain)

    def d_across(l, q):
        far_copy(q).wait_recv()
        sxd[l, q] = (sd[q, rows(DH * c, DH), :].astype(f32) + rd3d[q].astype(f32)).astype(bf16)
        xd_copy(l, q).start()
        drain(far_copy(q))

    def bring(n, part, act):
        act(pltpu.make_async_copy(part, h.at[n * 384 : (n + 1) * 384, :], fsem.at[n]))

    def put(n, dst, act):
        act(pltpu.make_async_copy(h.at[1152 + RB * n : 1152 + RB * (n + 1), :], dst, fout.at[n]))

    def add_up(parts, puts):
        for n, part in enumerate(parts):
            bring(n, part, drain)
        for r in range(0, 384, 128):
            g = h[r : r + 128, :].astype(f32) + h[384 + r : 512 + r, :].astype(f32) + h[768 + r : 896 + r, :].astype(f32)
            g = g.astype(bf16)
            h[1152 + r : 1280 + r, :] = g
            g = g.astype(f32)
            ssq[...] += jnp.sum((g * g).reshape(16, 8, D), axis=0)
        for n, dst in enumerate(puts):
            put(n, dst, start)

    def put_done():
        for n in range(2):
            put(n, gg_hbm.at[0, :, 0:C], drain)

    def arrival(l, k):
        return near_first(k) if l == ONE else far_between(k, 1 - xx)

    def gu_parts(l, k):
        j = arrival(l, k)
        return [p0_hbm.at[l, j], rd2_hbm.at[l, j], rx_hbm.at[l, j]]

    def bring_gu(l, k):
        j = arrival(l, k)
        parts = gu_parts(l, k)
        remote(sg.at[2], parts[1], d_s.at[1], d_r2.at[l, j], at_p).wait_recv()
        bring(0, parts[0], start)
        bring(1, parts[1], start)
        remote(sx.at[0], parts[2], x_s.at[0], x_r.at[l, j], at_x).wait_recv()
        bring(2, parts[2], start)

    def add_gu(l, k):
        j = arrival(l, k)
        add_up(gu_parts(l, k), [gg_hbm.at[l, :, cols(j)], gu_hbm.at[l, :, cols(j)]])

    def d_parts(l, half):
        r = rows(half * DH, DH)
        return [own_d.at[l, r, :], rd_d.at[l, r, :], rx_d.at[l, r, :]]

    def bring_d(l, half):
        parts = d_parts(l, half)
        remote(sxd.at[0, 0], parts[2], xd_s.at[0, 0], xd_r.at[l, half], at_x).wait_recv()
        for n, part in enumerate(parts):
            bring(n, part, start)

    def add_d(l, half):
        add_up(d_parts(l, half), [gd_hbm.at[l, rows(half * DH + RB * n, RB), :] for n in range(2)])

    def other_core_d(l):
        remote(sd.at[0], rd_d.at[l], dd_s.at[1, 0], d_rd.at[l], at_p).wait_recv()

    def through(gate, up, dact):
        dact = dact.astype(bf16).astype(f32)
        sig = jax.nn.sigmoid(gate)
        silu = gate * sig
        dgu_s[:, C:] = (dact * silu).astype(bf16)
        dgu_s[:, :C] = (dact * up * (sig + silu * (1.0 - sig))).astype(bf16)
        return (silu * up).astype(bf16)

    def backward_2(k, t):
        r, s = tile(t), k % 2
        gu = dot(a1[r, :], w_gu[s])
        act_s[...] = through(gu[:, :C], gu[:, C:], dot(do[r, :], w_d[s], NT))
        acc[r, :] += dot(dgu_s[...], w_gu[s], NT)
        acc_gu[...] += dot(a1[r, :], dgu_s[...], TN)
        acc_d[...] += dot(act_s[...], do[r, :], TN)

    def saved(j, t):
        return pltpu.make_async_copy(up_hbm.at[j, tile(t), :], up_s.at[t % 2], back.at[t % 2])

    def backward_1(k, t):
        r, s = tile(t), t % 2
        saved(far_first(k), t).wait()

        @pl.when(t < LAST)
        def _():
            saved(far_first(k), t + 1).start()

        @pl.when((t == LAST) & (k < LAST))
        def _():
            saved(far_first(k + 1), FIRST).start()

        through(up_s[s, :, :C], up_s[s, :, C:], dot(do[r, :], w_d[k % 2], NT))
        acc_gu[...] += dot(a0[r, :], dgu_s[...], TN)

    @pl.loop(0, 4)
    def _(k):
        stage(TWO, k, far_between(k), drain)
        far = (k == SECOND) | (k == THIRD)

        @pl.loop(0, T // TM)
        def _(t):
            backward_2(k, t)

            @pl.when((t == FIRST) & (k > FIRST))
            def _():
                gu_across(TWO, k - 1, far_between(k - 1))

            @pl.when((t == FIRST) & ((k == THIRD) | (k == LAST)))
            def _():
                d_across(TWO, k // 2 + k % 2 - 1)

            @at(t, FIRST, k, SECOND)
            def _():
                near_copy(TWO, 0, drain)

            @at(t, FIRST, k, FIRST)
            def _():
                forward_x(TWO, GU_3)
                forward_y(TWO, DOWN_1)

            @at(t, SECOND, k, FIRST)
            def _():
                forward_x(TWO, DOWN_2)
                forward_y(TWO, GU_3)

            @at(t, THIRD, k, FIRST)
            def _():
                forward_x(TWO, GU_4)
                forward_y(TWO, DOWN_2)
                landed(TWO, GU_2, DOWN_1)
                stage(TWO, SECOND, far_between(SECOND), start)

            @at(t, FIRST, k, SECOND)
            def _():
                forward_y(TWO, GU_4)

            @at(t, THIRD, k, SECOND)
            def _():
                landed(TWO, GU_3, DOWN_2)
                stage(TWO, THIRD, far_between(THIRD), start)

            @at(t, THIRD, k, THIRD)
            def _():
                landed(TWO, GU_4)
                stage(TWO, LAST, far_between(LAST), start)

            @at(t, THIRD, k, LAST)
            def _():
                stage_d(ONE, FIRST, far_first(FIRST), start)

        round_gu()
        round_d(k // 2)
        gu_copies(TWO, k, far_between(k), start)

        @pl.when(far)
        def _():
            far_copy(k // 2).start()

        @pl.when(jnp.logical_not(far))
        def _():
            near_copy(TWO, k // 2, start)

    def product(j, to):
        return pltpu.make_async_copy(act_hbm.at[j], to, ld.at[0])

    product(far_first(FIRST), a1).start()
    saved(far_first(FIRST), FIRST).start()

    @pl.loop(0, T // 256)
    def _(t):
        r = pl.ds(pl.multiple_of(t * 256, 256), 256)
        wide = h[r, :].astype(f32)
        scale = scale_of(wide)
        da = acc[r, :].astype(bf16).astype(f32)
        mix = jnp.sum(da * wide, -1, keepdims=True) * (scale * scale * scale / D)
        down = (da * scale - wide * mix).astype(bf16)
        do[r, :] = (do[r, :].astype(f32) + down.astype(f32)).astype(bf16)

    gu_across(TWO, LAST, far_between(LAST))
    near_copy(TWO, 1, drain)

    def down_grad(k, of, then, then_of):
        product(far_first(k), of).wait()
        if then is not None:
            product(far_first(then), then_of).start()

        @pl.loop(0, T // TM)
        def _(t):
            acc_d[...] += dot(of[tile(t), :], do[tile(t), :], TN)

    down_grad(FIRST, a1, SECOND, h)
    round_d(0)
    far_copy(0).start()
    down_grad(SECOND, h, THIRD, a1)
    d_across(ONE, 0)
    round_d(1)
    far_copy(1).start()
    down_grad(THIRD, a1, LAST, h)
    d_across(ONE, 1)
    round_d(0)
    near_copy(ONE, 0, start)
    down_grad(LAST, h, None, None)
    near_copy(ONE, 0, drain)
    round_d(1)
    near_copy(ONE, 1, start)

    @pl.loop(0, 4)
    def _(k):
        stage_d(ONE, k, far_first(k), drain)

        @pl.loop(0, T // TM)
        def _(t):
            backward_1(k, t)

            @at(t, FIRST, k, FIRST)
            def _():
                near_copy(ONE, 1, drain)
                other_core_d(TWO)

            @pl.when((t == FIRST) & ((k == SECOND) | (k == THIRD)))
            def _():
                add_d(TWO, k - 1)

            @pl.when((t == FIRST) & (k > FIRST))
            def _():
                put_done()

            @pl.when(t == FIRST)
            def _():
                bring_gu(TWO, k)

            @pl.when((t == SECOND) & (k > FIRST))
            def _():
                gu_across(ONE, k - 1, far_first(k - 1))

            @pl.when((t == SECOND) & (k < LAST))
            def _():
                stage_d(ONE, k + 1, far_first(k + 1), start)

            @pl.when(t == THIRD)
            def _():
                add_gu(TWO, k)

            @pl.when((t == LAST) & (k < THIRD))
            def _():
                put_done()
                bring_d(TWO, k)

        round_gu()
        gu_copies(ONE, k, far_first(k), start)

    gu_across(ONE, LAST, far_first(LAST))
    other_core_d(ONE)

    @pl.loop(0, 2)
    def _(half):
        put_done()
        bring_d(ONE, half)
        add_d(ONE, half)

    @pl.loop(0, 4)
    def _(k):
        put_done()
        bring_gu(ONE, k)
        add_gu(ONE, k)

    part = ssq[:, :128]
    for n in range(1, D // 128):
        part = part + ssq[:, n * 128 : (n + 1) * 128]
    ss_src[...] = part
    for l in range(L):
        for p in range(10):
            for which, (src, half, to) in enumerate(((ix, y, at_x), (ix, y, at_y), (ix, y, at_p), (ix, 1 - y, at_p))):
                if which == OVER_X:
                    send_x(l, p, drain)
                else:
                    r = mine(l, p, src, half)
                    remote(r, r, ag_s.at[l, p, which], ag_r.at[l, p, which], to).wait_send()
        for m in range(3):
            to_peer(l, m).wait_send()
        for q in range(2):
            xd_copy(l, q).wait_send()
    for k in range(4):
        x_copy(ONE, k, far_first(k)).wait_send()
    tells = [
        remote(ss_src, ss.at[i], ss_s.at[n], ss_r.at[i], to) for n, to in enumerate((at_x, at_p, at_q))
    ]
    for tell in tells:
        tell.start()
    for src in (ix, ip, iq):
        remote(ss_src, ss.at[src], ss_s.at[0], ss_r.at[src], at_x).wait_recv()
    for tell in tells:
        tell.wait_send()
    put_done()
    ss[i] = part
    total = jnp.sum(ss[0] + ss[1] + ss[2] + ss[3])
    fac[...] = jnp.minimum(1.0, 0.5 * lax.rsqrt(jnp.full((8, 128), total / COUNT + 1e-30, f32)))


def gradients(x, dy, wg, wu, wd):
    hbm = pl.BlockSpec(memory_space=pl.ANY)
    vmem = pl.BlockSpec(memory_space=pltpu.VMEM)
    out = lambda *shape: jax.ShapeDtypeStruct(shape, bf16)
    dma = lambda *shape: pltpu.SemaphoreType.DMA(shape)
    return pl.pallas_call(
        step_kernel,
        in_specs=[hbm] * 5,
        out_specs=[hbm] * 3 + [vmem] + [hbm] * 11,
        out_shape=[
            out(L, RB, FF), out(L, RB, FF), out(L, C, D), jax.ShapeDtypeStruct((8, 128), f32),
            out(L, D, FF), out(L, D, FF), out(L, FF, D),
            out(L, 4, 2 * RB, C), out(L, 4, 2 * RB, C), out(L, 4, 2 * RB, C),
            out(L, C, D), out(L, C, D), out(L, C, D),
            jax.ShapeDtypeStruct((4, T, 2 * C), f32), out(4, T, C),
        ],
        scratch_shapes=[
            pltpu.VMEM((T, D), bf16), pltpu.VMEM((T, D), bf16), pltpu.VMEM((T, D), bf16), pltpu.VMEM((T, D), bf16),
            pltpu.VMEM((T, D), f32), pltpu.VMEM((D, 2 * C), f32), pltpu.VMEM((C, D), f32),
            pltpu.VMEM((2, D, 2 * C), bf16), pltpu.VMEM((2, C, D), bf16),
            pltpu.VMEM((TM, C), bf16), pltpu.VMEM((TM, 2 * C), bf16),
            pltpu.VMEM((4, 2 * RB, C), bf16), pltpu.VMEM((2, C, D), bf16),
            pltpu.VMEM((2, 2 * RB, C), bf16), pltpu.VMEM((2, DH, D), bf16),
            pltpu.VMEM((4, 2 * RB, C), bf16), pltpu.VMEM((2, 2, DH, D), bf16),
            pltpu.VMEM((8, D), f32), pltpu.VMEM((4, 8, 128), f32), pltpu.VMEM((8, 128), f32), pltpu.VMEM((2, TM, 2 * C), f32),
            dma(L, 10, 4), dma(L, 10, 4), dma(L, 3), dma(L, 3), dma(2), dma(2, 7),
            dma(2), dma(2), dma(2, 2), dma(2), dma(L, 4), dma(L), dma(2), dma(4), dma(L, 4), dma(L, 2), dma(L, 2),
            dma(3), dma(2), dma(3), dma(4), dma(2, 2), dma(2),
        ],
        compiler_params=pltpu.CompilerParams(
            collective_id=0, has_side_effects=True, vmem_limit_bytes=63 * 2**20
        ),
        name="train_step",
    )(x, dy, wg, wu, wd)


def adamw_kernel(*refs):
    fac, ins, outs = refs[0], refs[1:13], refs[13:]
    factor = fac[0:1, 0:1]
    for n in range(3):
        g, w, m, v = (ins[3 * which + n] for which in range(4))
        grad = g[0].astype(f32) * factor
        new_m = 0.9 * m[0] + 0.1 * grad
        new_v = 0.95 * v[0] + 0.05 * grad * grad
        wide = w[0].astype(f32)
        outs[n][0] = (wide - 0.02 * (new_m * lax.rsqrt(new_v + 1e-8) + 0.1 * wide)).astype(bf16)
        outs[3 + n][0] = new_m
        outs[6 + n][0] = new_v


def adamw(factor, g, w, m, v):
    wide = pl.BlockSpec((1, RB // N, FF), lambda t: (t // N, t % N, 0))
    tall = pl.BlockSpec((1, C // N, D), lambda t: (t // N, t % N, 0))
    specs = [wide, wide, tall]
    shapes = lambda dtype: [jax.ShapeDtypeStruct(a.shape, dtype) for a in w]
    return pl.pallas_call(
        adamw_kernel,
        grid=(L * N,),
        in_specs=[pl.BlockSpec((8, 128), lambda t: (0, 0))] + specs * 4,
        out_specs=specs * 3,
        out_shape=shapes(bf16) + shapes(f32) + shapes(f32),
        compiler_params=pltpu.CompilerParams(vmem_limit_bytes=63 * 2**20),
        name="adamw",
    )(factor, *g, *w, *m, *v)


def solution(mesh):
    def step(x, dy, *arrays):
        w, m, v = (arrays[n : n + 3] for n in (0, 3, 6))
        gg, gu, gd, factor, *_ = gradients(x[0], dy[0], *w)
        return tuple(adamw(factor, (gg, gu, gd), w, m, v))

    states, cut = P(("rep", "dp"), None, None), P(None, "dp", None)
    return jax.shard_map(
        step,
        mesh=mesh,
        in_specs=(states, states) + (cut,) * 9,
        out_specs=(P("rep", "dp", None),) * 9,
        check_vma=False,
    )
```

```python
import functools

import jax
import jax.numpy as jnp
from jax import lax
from jax.experimental import pallas as pl
from jax.experimental.pallas import tpu as pltpu
from jax.sharding import PartitionSpec as P

T, D, FF, L = 2048, 768, 3072, 2
C = 768
TM = 512
RB = D // 4
RH = RB // 2
DH = C // 2
DQ = C // 4
N = 4
COUNT = 3 * L * D * FF
FIRST, SECOND, THIRD, LAST = range(4)
OVER_X, OVER_Y, TO_CORE, Y_TO_CORE = range(4)
GU = [(n, n + 1) for n in range(0, 8, 2)]
GU_1, GU_2, GU_3, GU_4 = GU
DOWN_1, DOWN_2 = (8,), (9,)
ONE, TWO = range(L)
bf16, f32 = jnp.bfloat16, jnp.float32
NT = (((1,), (1,)), ((), ()))
TN = (((0,), (0,)), ((), ()))
MESH = pl.DeviceIdType.MESH


def dot(a, b, dims=(((1,), (0,)), ((), ()))):
    return lax.dot_general(a, b, dims, preferred_element_type=f32)


def scale_of(wide):
    return lax.rsqrt(jnp.mean(wide * wide, -1, keepdims=True) + 1e-6)


def step_kernel(
    x_hbm, dy_hbm, wg, wu, wd,
    gg_hbm, gu_hbm, gd_hbm, fac, all_g, all_u, all_d, p0_hbm, rd2_hbm, rx_hbm, own_d, rd_d, rx_d, up_hbm, act_hbm,
    h, a0, a1, do, acc, acc_gu, acc_d, w_gu, w_d, act_s, dgu_s, sg, sd, rd3, rd3d, sx, sxd, ssq, ss, ss_src, up_s,
    ag_s, ag_r, pe_s, pe_r, ld, wsem, d_s, d_r3, dd_s, d_r3d, d_r2, d_rd, keep, x_s, x_r, xd_s, xd_r, fsem, fout, ss_s, ss_r, save, back,
):
    y, i = lax.axis_index("rep"), lax.axis_index("dp")
    xx, c = i // 2, i % 2
    ix, ip, iq = (1 - xx) * 2 + c, xx * 2 + 1 - c, (1 - xx) * 2 + 1 - c
    at_x, at_p, at_q, at_y = (y, ix), (y, ip), (y, iq), (1 - y, i)

    def remote(src, dst, send, recv, to):
        return pltpu.make_async_remote_copy(
            src_ref=src, dst_ref=dst, send_sem=send, recv_sem=recv, device_id=to, device_id_type=MESH
        )

    def near_first(k):
        return (2 * xx + k) % 4

    def far_first(k):
        return (2 * (1 - xx) + k) % 4

    def start(copy):
        copy.start()

    def drain(copy):
        copy.wait_send() if copy.is_remote else copy.wait()

    def duties(t, k, *work):
        for n in range(T // TM):
            here = [(m, f) for tile_n, m, f in work if tile_n == n]
            if here:

                @pl.when(t == n)
                def _():
                    for m, f in here:
                        if m is None:
                            f()
                        else:
                            pl.when(k == m)(f)

    def cols(j):
        return pl.ds(pl.multiple_of(j * C, C), C)

    def rows(start, size):
        return pl.ds(pl.multiple_of(start, 32), size)

    barrier = pltpu.get_barrier_semaphore()
    for other in (at_x, at_p, at_q, at_y):
        pl.semaphore_signal(barrier, inc=1, device_id=other, device_id_type=MESH)
    load_x = pltpu.make_async_copy(x_hbm, h, ld.at[0])
    load_dy = pltpu.make_async_copy(dy_hbm, do, ld.at[1])
    load_x.start()
    load_dy.start()
    pl.semaphore_wait(barrier, 4)

    def region(l, p, src, half, j):
        if p >= 8:
            return all_d.at[l, rows(C * (src // 2 * 2 + p - 8) + DH * half + DQ * (src % 2), DQ), :]
        return (all_g, all_u)[p % 2].at[l, rows(RB * src + RH * half, RH), cols(j)]

    def mine(l, p, src, half):
        return region(l, p, src, half, (near_first, far_first)[l](p // 2))

    def send_x(l, p, act):
        j = (far_first, near_first)[l](p // 2)
        there = region(l, p, i, y, j)

        def copy(src):
            return remote(src, there, ag_s.at[l, p, OVER_X], ag_r.at[l, p, OVER_X], at_x)

        if p < 8:
            act(copy((wg, wu)[p % 2].at[l, rows(RH * y, RH), cols(j)]))
        elif act is start:

            @pl.when(c == p - 8)
            def _():
                act(copy(wd.at[l, rows(DH * y + DQ * c, DQ), :]))

            @pl.when(c != p - 8)
            def _():
                act(copy(there))
        else:
            act(copy(there))

    def forward_x(l, *pieces):
        for p in sum(pieces, ()):
            r = mine(l, p, ix, y)
            remote(r, r, ag_s.at[l, p, OVER_X], ag_r.at[l, p, OVER_X], at_x).wait_recv()
            remote(r, r, ag_s.at[l, p, OVER_Y], ag_r.at[l, p, OVER_Y], at_y).start()
            remote(r, r, ag_s.at[l, p, TO_CORE], ag_r.at[l, p, TO_CORE], at_p).start()

    def forward_y(l, *pieces):
        for p in sum(pieces, ()):
            r = mine(l, p, ix, 1 - y)
            remote(r, r, ag_s.at[l, p, OVER_Y], ag_r.at[l, p, OVER_Y], at_y).wait_recv()
            remote(r, r, ag_s.at[l, p, Y_TO_CORE], ag_r.at[l, p, Y_TO_CORE], at_p).start()

    def landed(l, *pieces):
        for p in sum(pieces, ()):
            for which, half in ((TO_CORE, y), (Y_TO_CORE, 1 - y)):
                r = mine(l, p, iq, half)
                remote(r, r, ag_s.at[l, p, which], ag_r.at[l, p, which], at_p).wait_recv()

    def to_peer(l, m):
        src = (wg, wu, wd)[m].at[l]
        dst = (all_g.at[l, rows(RB * i, RB), :], all_u.at[l, rows(RB * i, RB), :], all_d.at[l, rows(C * i, C), :])[m]
        return remote(src, dst, pe_s.at[l, m], pe_r.at[l, m], at_p)

    def from_peer(l):
        for m in range(3):
            to_peer(l, m).wait_recv()

    def send(l, *pieces):
        for p in sum(pieces, ()):
            send_x(l, p, start)

    send(ONE, GU_1, GU_2, GU_3)
    for l in range(L):
        for m in range(3):
            to_peer(l, m).start()

    def stage_gu(l, k, j, act):
        slot = k % 2
        for m, (own, gathered) in enumerate(((wg, all_g), (wu, all_u))):
            for n, (src, row, size) in enumerate(
                (
                    (own.at[l, :, cols(j)], RB * i, RB),
                    (gathered.at[l, rows(RB * ip, RB), cols(j)], RB * ip, RB),
                    (gathered.at[l, rows(2 * RB * (1 - xx), 2 * RB), cols(j)], 2 * RB * (1 - xx), 2 * RB),
                )
            ):
                copy = pltpu.make_async_copy(
                    src, w_gu.at[slot, rows(row, size), m * C : (m + 1) * C], wsem.at[slot, 3 * m + n]
                )
                act(copy)

    def stage_d(l, k, j, act):
        slot = k % 2
        theirs = pltpu.make_async_copy(all_d.at[l, rows(C * j, C), :], w_d.at[slot], wsem.at[slot, 6])
        if act is start:

            @pl.when(j == i)
            def _():
                pltpu.make_async_copy(wd.at[l], w_d.at[slot], wsem.at[slot, 6]).start()

            @pl.when(j != i)
            def _():
                theirs.start()
        else:
            act(theirs)

    def stage(l, k, j, act):
        stage_gu(l, k, j, act)
        stage_d(l, k, j, act)

    def tile(t):
        return pl.ds(pl.multiple_of(t * TM, TM), TM)

    def clear(ref, size):
        n = ref.shape[0] // size

        @pl.loop(0, n)
        def _(t):
            ref[pl.ds(pl.multiple_of(t * size, size), size), :] = jnp.zeros((size, ref.shape[1]), ref.dtype)

    clear(acc, 256)
    clear(acc_gu, 128)
    clear(acc_d, 128)
    ssq[...] = jnp.zeros_like(ssq)
    load_x.wait()

    @pl.loop(0, T // 256)
    def _(t):
        r = pl.ds(pl.multiple_of(t * 256, 256), 256)
        wide = h[r, :].astype(f32)
        a0[r, :] = (wide * scale_of(wide)).astype(bf16)

    def saving(j, t, act):
        s = t % 2
        act(pltpu.make_async_copy(up_s.at[s], up_hbm.at[j, tile(t), :], save.at[0, s]))
        act(pltpu.make_async_copy(dgu_s.at[:, cols(s)], act_hbm.at[j, tile(t), :], save.at[1, s]))

    def forward(k, t):
        r, s = tile(t), t % 2

        @pl.when((k > 0) | (t > 1))
        def _():
            saving(near_first(k), t, drain)

        gu = dot(a0[r, :], w_gu[k % 2])
        up_s[s] = gu
        gate, up = gu[:, :C], gu[:, C:]
        act = (gate * jax.nn.sigmoid(gate) * up).astype(bf16)
        dgu_s[:, cols(s)] = act
        saving(near_first(k), t, start)
        acc[r, :] += dot(act, w_d[k % 2])

    forward_x(ONE, GU_1)
    from_peer(ONE)
    send(ONE, DOWN_1, GU_4, DOWN_2)
    forward_x(ONE, GU_2)
    forward_y(ONE, GU_1)
    landed(ONE, GU_1)
    stage(ONE, FIRST, near_first(FIRST), start)

    def begin():
        from_peer(TWO)
        send(TWO, GU_1, DOWN_1, GU_2, DOWN_2, GU_3, GU_4)
        forward_x(ONE, GU_3[:1])

    def ready_gu(l, k, j, *pieces):
        landed(l, *pieces)
        stage_gu(l, k, j, start)

    def ready_d(l, k, j, *pieces):
        landed(l, *pieces)
        stage_d(l, k, j, start)

    def ready(l, k, j, *pieces):
        landed(l, *pieces)
        stage(l, k, j, start)

    def later(f, *args):
        return lambda: f(*args)

    def pass_later(*args):
        def go():
            for f, *rest in args:
                f(*rest)

        return go

    X, Y = forward_x, forward_y

    @pl.loop(0, 4)
    def _(k):
        stage(ONE, k, near_first(k), drain)

        @pl.loop(0, T // TM)
        def _(t):
            forward(k, t)
            duties(
                t, k,
                (FIRST, FIRST, begin),
                (SECOND, FIRST, pass_later((X, ONE, GU_3[1:]), (Y, ONE, GU_2))),
                (THIRD, FIRST, later(ready, ONE, SECOND, near_first(SECOND), GU_2)),
                (FIRST, SECOND, pass_later((X, ONE, DOWN_1), (Y, ONE, GU_3))),
                (SECOND, SECOND, pass_later((X, ONE, GU_4[:1]))),
                (SECOND, SECOND, later(ready_gu, ONE, THIRD, near_first(THIRD), GU_3)),
                (THIRD, SECOND, pass_later((X, ONE, GU_4[1:]), (Y, ONE, DOWN_1))),
                (LAST, SECOND, later(ready_d, ONE, THIRD, near_first(THIRD), DOWN_1)),
                (FIRST, THIRD, pass_later((X, ONE, DOWN_2), (Y, ONE, GU_4))),
                (SECOND, THIRD, later(ready_gu, ONE, LAST, near_first(LAST), GU_4)),
                (THIRD, THIRD, pass_later((X, TWO, GU_1[:1]))),
                (LAST, THIRD, pass_later((X, TWO, GU_1[1:]), (Y, ONE, DOWN_2))),
                (LAST, THIRD, later(ready_d, ONE, LAST, near_first(LAST), DOWN_2)),
                (FIRST, LAST, pass_later((X, TWO, DOWN_1), (Y, TWO, GU_1))),
                (SECOND, LAST, later(ready_gu, TWO, FIRST, far_first(FIRST), GU_1)),
                (THIRD, LAST, pass_later((X, TWO, GU_2[:1]))),
                (LAST, LAST, pass_later((X, TWO, GU_2[1:]), (Y, TWO, DOWN_1))),
            )

    load_dy.wait()
    for n in (THIRD, LAST):
        saving(near_first(LAST), n, drain)

    @pl.loop(0, T // 256)
    def _(t):
        r = pl.ds(pl.multiple_of(t * 256, 256), 256)
        wide = (h[r, :].astype(f32) + acc[r, :].astype(bf16).astype(f32)).astype(bf16)
        h[r, :] = wide
        wide = wide.astype(f32)
        a1[r, :] = (wide * scale_of(wide)).astype(bf16)
        acc[r, :] = jnp.zeros((256, D), f32)

        @pl.when(t == SECOND)
        def _():
            ready_d(TWO, FIRST, far_first(FIRST), DOWN_1)


    def gu_copies(l, k, j, act):
        act(remote(sg.at[3], rd3.at[k % 2], d_s.at[0], d_r3.at[k % 2], at_p))
        act(remote(sg.at[2], rd2_hbm.at[l, j], d_s.at[1], d_r2.at[l, j], at_p))
        act(pltpu.make_async_copy(sg.at[0], p0_hbm.at[l, j], keep.at[0]))

    def far_copy(q):
        return remote(sd.at[q, rows(DH * (1 - c), DH), :], rd3d.at[q], dd_s.at[0, q], d_r3d.at[q], at_p)

    def near_copy(l, q, act):
        @pl.when(c != q)
        def _():
            act(remote(sd.at[q], rd_d.at[l], dd_s.at[1, q], d_rd.at[l], at_p))

        @pl.when(c == q)
        def _():
            act(pltpu.make_async_copy(sd.at[q], own_d.at[l], keep.at[1]))

    def round_gu():
        for r, dest in ((3, iq), (1, ix), (2, ip), (0, i)):
            for m in range(2):
                sg[r, RB * m : RB * (m + 1), :] = acc_gu[rows(RB * dest, RB), m * C : (m + 1) * C].astype(bf16)
        clear(acc_gu, 128)

    def round_d(q):
        sd[q] = acc_d[...].astype(bf16)
        clear(acc_d, 128)

    def x_copy(l, k, j):
        return remote(sx.at[k], rx_hbm.at[l, j], x_s.at[k], x_r.at[l, j], at_x)

    def xd_copy(l, q):
        return remote(sxd.at[l, q], rx_d.at[l, rows(DH * c, DH), :], xd_s.at[l, q], xd_r.at[l, c], (y, 2 * (1 - xx) + q))

    def gu_across(l, k, j):
        remote(sg.at[3], rd3.at[k % 2], d_s.at[0], d_r3.at[k % 2], at_p).wait_recv()
        if l == ONE:
            x_copy(l, k, j).wait_send()
        sx[k] = (sg[1].astype(f32) + rd3[k % 2].astype(f32)).astype(bf16)
        x_copy(l, k, j).start()
        gu_copies(l, k, j, drain)

    def d_across(l, q):
        far_copy(q).wait_recv()
        sxd[l, q] = (sd[q, rows(DH * c, DH), :].astype(f32) + rd3d[q].astype(f32)).astype(bf16)
        xd_copy(l, q).start()
        drain(far_copy(q))

    def bring(n, part, act):
        act(pltpu.make_async_copy(part, h.at[n * 384 : (n + 1) * 384, :], fsem.at[n]))

    def put(n, dst, act):
        act(pltpu.make_async_copy(h.at[1152 + RB * n : 1152 + RB * (n + 1), :], dst, fout.at[n]))

    def add_up(parts, puts):
        for n, part in enumerate(parts):
            bring(n, part, drain)
        for r in range(0, 384, 128):
            g = h[r : r + 128, :].astype(f32) + h[384 + r : 512 + r, :].astype(f32) + h[768 + r : 896 + r, :].astype(f32)
            g = g.astype(bf16)
            h[1152 + r : 1280 + r, :] = g
            g = g.astype(f32)
            ssq[...] += jnp.sum((g * g).reshape(16, 8, D), axis=0)
        for n, dst in enumerate(puts):
            put(n, dst, start)

    def put_done():
        for n in range(2):
            put(n, gg_hbm.at[0, :, 0:C], drain)

    def gu_parts(l, k):
        j = near_first(k)
        return [p0_hbm.at[l, j], rd2_hbm.at[l, j], rx_hbm.at[l, j]]

    def bring_gu(l, k):
        j = near_first(k)
        parts = gu_parts(l, k)
        remote(sg.at[2], parts[1], d_s.at[1], d_r2.at[l, j], at_p).wait_recv()
        bring(0, parts[0], start)
        bring(1, parts[1], start)
        remote(sx.at[0], parts[2], x_s.at[0], x_r.at[l, j], at_x).wait_recv()
        bring(2, parts[2], start)

    def add_gu(l, k):
        j = near_first(k)
        add_up(gu_parts(l, k), [gg_hbm.at[l, :, cols(j)], gu_hbm.at[l, :, cols(j)]])

    def d_parts(l, half):
        r = rows(half * DH, DH)
        return [own_d.at[l, r, :], rd_d.at[l, r, :], rx_d.at[l, r, :]]

    def bring_d(l, half):
        parts = d_parts(l, half)
        remote(sxd.at[0, 0], parts[2], xd_s.at[0, 0], xd_r.at[l, half], at_x).wait_recv()
        for n, part in enumerate(parts):
            bring(n, part, start)

    def add_d(l, half):
        add_up(d_parts(l, half), [gd_hbm.at[l, rows(half * DH + RB * n, RB), :] for n in range(2)])

    def other_core_d(l):
        remote(sd.at[0], rd_d.at[l], dd_s.at[1, 0], d_rd.at[l], at_p).wait_recv()

    def through(gate, up, dact):
        dact = dact.astype(bf16).astype(f32)
        sig = jax.nn.sigmoid(gate)
        silu = gate * sig
        dgu_s[:, C:] = (dact * silu).astype(bf16)
        dgu_s[:, :C] = (dact * up * (sig + silu * (1.0 - sig))).astype(bf16)
        return (silu * up).astype(bf16)

    def backward_2(k, t):
        r, s = tile(t), k % 2
        gu = dot(a1[r, :], w_gu[s])
        act_s[...] = through(gu[:, :C], gu[:, C:], dot(do[r, :], w_d[s], NT))
        acc[r, :] += dot(dgu_s[...], w_gu[s], NT)
        acc_gu[...] += dot(a1[r, :], dgu_s[...], TN)
        acc_d[...] += dot(act_s[...], do[r, :], TN)

    def saved(j, t):
        return pltpu.make_async_copy(up_hbm.at[j, tile(t), :], up_s.at[t % 2], back.at[t % 2])

    def backward_1(k, t):
        r, s = tile(t), t % 2
        saved(far_first(k), t).wait()

        @pl.when(t < LAST)
        def _():
            saved(far_first(k), t + 1).start()

        @pl.when((t == LAST) & (k < LAST))
        def _():
            saved(far_first(k + 1), FIRST).start()

        through(up_s[s, :, :C], up_s[s, :, C:], dot(do[r, :], w_d[k % 2], NT))
        acc_gu[...] += dot(a0[r, :], dgu_s[...], TN)

    @pl.loop(0, 4)
    def _(k):
        stage(TWO, k, far_first(k), drain)

        @pl.loop(0, T // TM)
        def _(t):
            backward_2(k, t)

            def sums():
                @pl.when(k > FIRST)
                def _():
                    gu_across(TWO, k - 1, far_first(k - 1))

                @pl.when((k == SECOND) | (k == THIRD))
                def _():
                    d_across(TWO, k - 1)

            duties(
                t, k,
                (FIRST, None, sums),
                (FIRST, FIRST, pass_later((X, TWO, DOWN_2), (Y, TWO, GU_2))),
                (SECOND, FIRST, pass_later((X, TWO, GU_3), (Y, TWO, DOWN_2))),
                (THIRD, FIRST, pass_later((X, TWO, GU_4))),
                (THIRD, FIRST, later(ready, TWO, SECOND, far_first(SECOND), GU_2, DOWN_2)),
                (LAST, FIRST, pass_later((Y, TWO, GU_3))),
                (FIRST, SECOND, pass_later((Y, TWO, GU_4))),
                (THIRD, SECOND, later(ready, TWO, THIRD, far_first(THIRD), GU_3)),
                (THIRD, THIRD, later(ready, TWO, LAST, far_first(LAST), GU_4)),
                (FIRST, LAST, later(near_copy, TWO, 0, drain)),
                (THIRD, LAST, later(stage_d, ONE, FIRST, far_first(FIRST), start)),
            )

        round_gu()
        round_d(k % 2)
        gu_copies(TWO, k, far_first(k), start)

        @pl.when(k < THIRD)
        def _():
            far_copy(k).start()

        @pl.when(k >= THIRD)
        def _():
            near_copy(TWO, k - 2, start)

    def product(j, to):
        return pltpu.make_async_copy(act_hbm.at[j], to, ld.at[0])

    product(far_first(FIRST), a1).start()
    saved(far_first(FIRST), FIRST).start()

    @pl.loop(0, T // 256)
    def _(t):
        r = pl.ds(pl.multiple_of(t * 256, 256), 256)
        wide = h[r, :].astype(f32)
        scale = scale_of(wide)
        da = acc[r, :].astype(bf16).astype(f32)
        mix = jnp.sum(da * wide, -1, keepdims=True) * (scale * scale * scale / D)
        down = (da * scale - wide * mix).astype(bf16)
        do[r, :] = (do[r, :].astype(f32) + down.astype(f32)).astype(bf16)

    gu_across(TWO, LAST, far_first(LAST))

    def down_grad(k, of, then, then_of):
        product(far_first(k), of).wait()
        if then is not None:
            product(far_first(then), then_of).start()

        @pl.loop(0, T // TM)
        def _(t):
            acc_d[...] += dot(of[tile(t), :], do[tile(t), :], TN)

    down_grad(FIRST, a1, SECOND, h)
    round_d(0)
    far_copy(0).start()
    down_grad(SECOND, h, THIRD, a1)
    near_copy(TWO, 1, drain)
    d_across(ONE, 0)
    round_d(1)
    far_copy(1).start()
    down_grad(THIRD, a1, LAST, h)
    d_across(ONE, 1)
    round_d(0)
    near_copy(ONE, 0, start)
    down_grad(LAST, h, None, None)
    near_copy(ONE, 0, drain)
    round_d(1)
    near_copy(ONE, 1, start)

    @pl.loop(0, 4)
    def _(k):
        stage_d(ONE, k, far_first(k), drain)

        @pl.loop(0, T // TM)
        def _(t):
            backward_1(k, t)

            def fetch():
                @pl.when(k == FIRST)
                def _():
                    near_copy(ONE, 1, drain)
                    other_core_d(TWO)

                @pl.when((k == SECOND) | (k == THIRD))
                def _():
                    add_d(TWO, k - 1)

                @pl.when(k > FIRST)
                def _():
                    put_done()

                bring_gu(TWO, k)

            def sums():
                @pl.when(k > FIRST)
                def _():
                    gu_across(ONE, k - 1, far_first(k - 1))

                @pl.when(k < LAST)
                def _():
                    stage_d(ONE, k + 1, far_first(k + 1), start)

            def fetch_d():
                @pl.when(k < THIRD)
                def _():
                    put_done()
                    bring_d(TWO, k)

            duties(
                t, k,
                (FIRST, None, fetch),
                (SECOND, None, sums),
                (THIRD, None, later(add_gu, TWO, k)),
                (LAST, None, fetch_d),
            )

        round_gu()
        gu_copies(ONE, k, far_first(k), start)

    gu_across(ONE, LAST, far_first(LAST))
    other_core_d(ONE)

    @pl.loop(0, 2)
    def _(half):
        put_done()
        bring_d(ONE, half)
        add_d(ONE, half)

    @pl.loop(0, 4)
    def _(k):
        put_done()
        bring_gu(ONE, k)
        add_gu(ONE, k)

    part = ssq[:, :128]
    for n in range(1, D // 128):
        part = part + ssq[:, n * 128 : (n + 1) * 128]
    ss_src[...] = part
    for l in range(L):
        for p in range(10):
            for which, (src, half, to) in enumerate(((ix, y, at_x), (ix, y, at_y), (ix, y, at_p), (ix, 1 - y, at_p))):
                if which == OVER_X:
                    send_x(l, p, drain)
                else:
                    r = mine(l, p, src, half)
                    remote(r, r, ag_s.at[l, p, which], ag_r.at[l, p, which], to).wait_send()
        for m in range(3):
            to_peer(l, m).wait_send()
        for q in range(2):
            xd_copy(l, q).wait_send()
    for k in range(4):
        x_copy(ONE, k, far_first(k)).wait_send()
    tells = [
        remote(ss_src, ss.at[i], ss_s.at[n], ss_r.at[i], to) for n, to in enumerate((at_x, at_p, at_q))
    ]
    for tell in tells:
        tell.start()
    for src in (ix, ip, iq):
        remote(ss_src, ss.at[src], ss_s.at[0], ss_r.at[src], at_x).wait_recv()
    for tell in tells:
        tell.wait_send()
    put_done()
    ss[i] = part
    total = jnp.sum(ss[0] + ss[1] + ss[2] + ss[3])
    fac[...] = jnp.minimum(1.0, 0.5 * lax.rsqrt(jnp.full((8, 128), total / COUNT + 1e-30, f32)))


def gradients(x, dy, wg, wu, wd):
    hbm = pl.BlockSpec(memory_space=pl.ANY)
    vmem = pl.BlockSpec(memory_space=pltpu.VMEM)
    out = lambda *shape: jax.ShapeDtypeStruct(shape, bf16)
    dma = lambda *shape: pltpu.SemaphoreType.DMA(shape)
    return pl.pallas_call(
        step_kernel,
        in_specs=[hbm] * 5,
        out_specs=[hbm] * 3 + [vmem] + [hbm] * 11,
        out_shape=[
            out(L, RB, FF), out(L, RB, FF), out(L, C, D), jax.ShapeDtypeStruct((8, 128), f32),
            out(L, D, FF), out(L, D, FF), out(L, FF, D),
            out(L, 4, 2 * RB, C), out(L, 4, 2 * RB, C), out(L, 4, 2 * RB, C),
            out(L, C, D), out(L, C, D), out(L, C, D),
            jax.ShapeDtypeStruct((4, T, 2 * C), f32), out(4, T, C),
        ],
        scratch_shapes=[
            pltpu.VMEM((T, D), bf16), pltpu.VMEM((T, D), bf16), pltpu.VMEM((T, D), bf16), pltpu.VMEM((T, D), bf16),
            pltpu.VMEM((T, D), f32), pltpu.VMEM((D, 2 * C), f32), pltpu.VMEM((C, D), f32),
            pltpu.VMEM((2, D, 2 * C), bf16), pltpu.VMEM((2, C, D), bf16),
            pltpu.VMEM((TM, C), bf16), pltpu.VMEM((TM, 2 * C), bf16),
            pltpu.VMEM((4, 2 * RB, C), bf16), pltpu.VMEM((2, C, D), bf16),
            pltpu.VMEM((2, 2 * RB, C), bf16), pltpu.VMEM((2, DH, D), bf16),
            pltpu.VMEM((4, 2 * RB, C), bf16), pltpu.VMEM((2, 2, DH, D), bf16),
            pltpu.VMEM((8, D), f32), pltpu.VMEM((4, 8, 128), f32), pltpu.VMEM((8, 128), f32), pltpu.VMEM((2, TM, 2 * C), f32),
            dma(L, 10, 4), dma(L, 10, 4), dma(L, 3), dma(L, 3), dma(2), dma(2, 7),
            dma(2), dma(2), dma(2, 2), dma(2), dma(L, 4), dma(L), dma(2), dma(4), dma(L, 4), dma(L, 2), dma(L, 2),
            dma(3), dma(2), dma(3), dma(4), dma(2, 2), dma(2),
        ],
        compiler_params=pltpu.CompilerParams(
            collective_id=0, has_side_effects=True, vmem_limit_bytes=63 * 2**20
        ),
        name="train_step",
    )(x, dy, wg, wu, wd)


def adamw_kernel(*refs):
    fac, ins, outs = refs[0], refs[1:13], refs[13:]
    factor = fac[0:1, 0:1]
    for n in range(3):
        g, w, m, v = (ins[3 * which + n] for which in range(4))
        grad = g[0].astype(f32) * factor
        new_m = 0.9 * m[0] + 0.1 * grad
        new_v = 0.95 * v[0] + 0.05 * grad * grad
        wide = w[0].astype(f32)
        outs[n][0] = (wide - 0.02 * (new_m * lax.rsqrt(new_v + 1e-8) + 0.1 * wide)).astype(bf16)
        outs[3 + n][0] = new_m
        outs[6 + n][0] = new_v


def adamw(factor, g, w, m, v):
    wide = pl.BlockSpec((1, RB // N, FF), lambda t: (t // N, t % N, 0))
    tall = pl.BlockSpec((1, C // N, D), lambda t: (t // N, t % N, 0))
    specs = [wide, wide, tall]
    shapes = lambda dtype: [jax.ShapeDtypeStruct(a.shape, dtype) for a in w]
    return pl.pallas_call(
        adamw_kernel,
        grid=(L * N,),
        in_specs=[pl.BlockSpec((8, 128), lambda t: (0, 0))] + specs * 4,
        out_specs=specs * 3,
        out_shape=shapes(bf16) + shapes(f32) + shapes(f32),
        compiler_params=pltpu.CompilerParams(vmem_limit_bytes=63 * 2**20),
        name="adamw",
    )(factor, *g, *w, *m, *v)


def solution(mesh):
    def step(x, dy, *arrays):
        w, m, v = (arrays[n : n + 3] for n in (0, 3, 6))
        gg, gu, gd, factor, *_ = gradients(x[0], dy[0], *w)
        return tuple(adamw(factor, (gg, gu, gd), w, m, v))

    states, cut = P(("rep", "dp"), None, None), P(None, "dp", None)
    return jax.shard_map(
        step,
        mesh=mesh,
        in_specs=(states, states) + (cut,) * 9,
        out_specs=(P("rep", "dp", None),) * 9,
        check_vma=False,
    )
```

```python
import functools

import jax
import jax.numpy as jnp
from jax import lax
from jax.experimental import pallas as pl
from jax.experimental.pallas import tpu as pltpu
from jax.sharding import PartitionSpec as P

T, D, FF, L = 2048, 768, 3072, 2
C = 768
TM = 512
RB = D // 4
RH = RB // 2
DH = C // 2
DQ = C // 4
ADAMW = 40
MEGA = 40
COUNT = 3 * L * D * FF
FIRST, SECOND, THIRD, LAST = range(4)
OVER_X, OVER_Y, TO_CORE, Y_TO_CORE = range(4)
GU = [(n, n + 1) for n in range(0, 8, 2)]
GU_1, GU_2, GU_3, GU_4 = GU
DOWN_1, DOWN_2 = (8,), (9,)
ONE, TWO = range(L)
bf16, f32 = jnp.bfloat16, jnp.float32
NT = (((1,), (1,)), ((), ()))
TN = (((0,), (0,)), ((), ()))
MESH = pl.DeviceIdType.MESH


def dot(a, b, dims=(((1,), (0,)), ((), ()))):
    return lax.dot_general(a, b, dims, preferred_element_type=f32)


def scale_of(wide):
    return lax.rsqrt(jnp.mean(wide * wide, -1, keepdims=True) + 1e-6)


def step_kernel(
    x_hbm, dy_hbm, wg, wu, wd, m_gate, m_up, m_down,
    gg_hbm, gu_hbm, gd_hbm, fac, all_g, all_u, all_d, p0_hbm, rd2_hbm, rx_hbm, own_d, rd_d, rx_d, up_hbm, act_hbm,
    acc, acc_gu, up_s, w_gu, w_d,
    h, a0, a1, do, acc_d, act_s, dgu_s, sg, sd, rd3, rd3d, sx, sxd, ssq, ss, ss_src,
    ag_s, ag_r, pe_s, pe_r, ld, wsem, d_s, d_r3, dd_s, d_r3d, d_r2, d_rd, keep, x_s, x_r, xd_s, xd_r, fsem, fout, ss_s, ss_r, save, back, early, late,
):
    y, i = lax.axis_index("rep"), lax.axis_index("dp")
    xx, c = i // 2, i % 2
    ix, ip, iq = (1 - xx) * 2 + c, xx * 2 + 1 - c, (1 - xx) * 2 + 1 - c
    at_x, at_p, at_q, at_y = (y, ix), (y, ip), (y, iq), (1 - y, i)

    def remote(src, dst, send, recv, to):
        return pltpu.make_async_remote_copy(
            src_ref=src, dst_ref=dst, send_sem=send, recv_sem=recv, device_id=to, device_id_type=MESH
        )

    def near_first(k):
        return (2 * xx + k) % 4

    def far_first(k):
        return (2 * (1 - xx) + k) % 4

    def start(copy):
        copy.start()

    def drain(copy):
        copy.wait_send() if copy.is_remote else copy.wait()

    def duties(t, k, *work):
        for n in range(T // TM):
            here = [(m, f) for tile_n, m, f in work if tile_n == n]
            if here:

                @pl.when(t == n)
                def _():
                    for m, f in here:
                        if m is None:
                            f()
                        else:
                            pl.when(k == m)(f)

    def cols(j):
        return pl.ds(pl.multiple_of(j * C, C), C)

    def rows(start, size):
        return pl.ds(pl.multiple_of(start, 32), size)

    barrier = pltpu.get_barrier_semaphore()
    for other in (at_x, at_p, at_q, at_y):
        pl.semaphore_signal(barrier, inc=1, device_id=other, device_id_type=MESH)
    load_x = pltpu.make_async_copy(x_hbm, h, ld.at[0])
    load_dy = pltpu.make_async_copy(dy_hbm, do, ld.at[1])
    load_x.start()
    load_dy.start()
    pl.semaphore_wait(barrier, 4)

    def region(l, p, src, half, j):
        if p >= 8:
            return all_d.at[l, rows(C * (src // 2 * 2 + p - 8) + DH * half + DQ * (src % 2), DQ), :]
        return (all_g, all_u)[p % 2].at[l, rows(RB * src + RH * half, RH), cols(j)]

    def mine(l, p, src, half):
        return region(l, p, src, half, (near_first, far_first)[l](p // 2))

    def send_x(l, p, act):
        j = (far_first, near_first)[l](p // 2)
        there = region(l, p, i, y, j)

        def copy(src):
            return remote(src, there, ag_s.at[l, p, OVER_X], ag_r.at[l, p, OVER_X], at_x)

        if p < 8:
            act(copy((wg, wu)[p % 2].at[l, rows(RH * y, RH), cols(j)]))
        elif act is start:

            @pl.when(c == p - 8)
            def _():
                act(copy(wd.at[l, rows(DH * y + DQ * c, DQ), :]))

            @pl.when(c != p - 8)
            def _():
                act(copy(there))
        else:
            act(copy(there))

    def forward_x(l, *pieces):
        for p in sum(pieces, ()):
            r = mine(l, p, ix, y)
            remote(r, r, ag_s.at[l, p, OVER_X], ag_r.at[l, p, OVER_X], at_x).wait_recv()
            remote(r, r, ag_s.at[l, p, OVER_Y], ag_r.at[l, p, OVER_Y], at_y).start()
            remote(r, r, ag_s.at[l, p, TO_CORE], ag_r.at[l, p, TO_CORE], at_p).start()

    def forward_y(l, *pieces):
        for p in sum(pieces, ()):
            r = mine(l, p, ix, 1 - y)
            remote(r, r, ag_s.at[l, p, OVER_Y], ag_r.at[l, p, OVER_Y], at_y).wait_recv()
            remote(r, r, ag_s.at[l, p, Y_TO_CORE], ag_r.at[l, p, Y_TO_CORE], at_p).start()

    def landed(l, *pieces):
        for p in sum(pieces, ()):
            for which, half in ((TO_CORE, y), (Y_TO_CORE, 1 - y)):
                r = mine(l, p, iq, half)
                remote(r, r, ag_s.at[l, p, which], ag_r.at[l, p, which], at_p).wait_recv()

    def to_peer(l, m):
        src = (wg, wu, wd)[m].at[l]
        dst = (all_g.at[l, rows(RB * i, RB), :], all_u.at[l, rows(RB * i, RB), :], all_d.at[l, rows(C * i, C), :])[m]
        return remote(src, dst, pe_s.at[l, m], pe_r.at[l, m], at_p)

    def from_peer(l):
        for m in range(3):
            to_peer(l, m).wait_recv()

    def send(l, *pieces):
        for p in sum(pieces, ()):
            send_x(l, p, start)

    send(ONE, GU_1, GU_2, GU_3)
    for l in range(L):
        for m in range(3):
            to_peer(l, m).start()

    def stage_gu(l, k, j, act):
        slot = k % 2
        for m, (own, gathered) in enumerate(((wg, all_g), (wu, all_u))):
            for n, (src, row, size) in enumerate(
                (
                    (own.at[l, :, cols(j)], RB * i, RB),
                    (gathered.at[l, rows(RB * ip, RB), cols(j)], RB * ip, RB),
                    (gathered.at[l, rows(2 * RB * (1 - xx), 2 * RB), cols(j)], 2 * RB * (1 - xx), 2 * RB),
                )
            ):
                copy = pltpu.make_async_copy(
                    src, w_gu.at[slot, rows(row, size), m * C : (m + 1) * C], wsem.at[slot, 3 * m + n]
                )
                act(copy)

    def stage_d(l, k, j, act):
        slot = k % 2
        theirs = pltpu.make_async_copy(all_d.at[l, rows(C * j, C), :], w_d.at[slot], wsem.at[slot, 6])
        if act is start:

            @pl.when(j == i)
            def _():
                pltpu.make_async_copy(wd.at[l], w_d.at[slot], wsem.at[slot, 6]).start()

            @pl.when(j != i)
            def _():
                theirs.start()
        else:
            act(theirs)

    def stage(l, k, j, act):
        stage_gu(l, k, j, act)
        stage_d(l, k, j, act)

    def tile(t):
        return pl.ds(pl.multiple_of(t * TM, TM), TM)

    def clear(ref, size):
        n = ref.shape[0] // size

        @pl.loop(0, n)
        def _(t):
            ref[pl.ds(pl.multiple_of(t * size, size), size), :] = jnp.zeros((size, ref.shape[1]), ref.dtype)

    clear(acc, 256)
    clear(acc_gu, 128)
    clear(acc_d, 128)
    ssq[...] = jnp.zeros_like(ssq)
    load_x.wait()

    @pl.loop(0, T // 256)
    def _(t):
        r = pl.ds(pl.multiple_of(t * 256, 256), 256)
        wide = h[r, :].astype(f32)
        a0[r, :] = (wide * scale_of(wide)).astype(bf16)

    def saving(j, t, act):
        s = t % 2
        act(pltpu.make_async_copy(up_s.at[s], up_hbm.at[j, tile(t), :], save.at[0, s]))
        act(pltpu.make_async_copy(dgu_s.at[:, cols(s)], act_hbm.at[j, tile(t), :], save.at[1, s]))

    def forward(k, t):
        r, s = tile(t), t % 2

        @pl.when((k > 0) | (t > 1))
        def _():
            saving(near_first(k), t, drain)

        gu = dot(a0[r, :], w_gu[k % 2])
        up_s[s] = gu
        gate, up = gu[:, :C], gu[:, C:]
        act = (gate * jax.nn.sigmoid(gate) * up).astype(bf16)
        dgu_s[:, cols(s)] = act
        saving(near_first(k), t, start)
        acc[r, :] += dot(act, w_d[k % 2])

    forward_x(ONE, GU_1)
    from_peer(ONE)
    send(ONE, DOWN_1, GU_4, DOWN_2)
    forward_x(ONE, GU_2)
    forward_y(ONE, GU_1)
    landed(ONE, GU_1)
    stage(ONE, FIRST, near_first(FIRST), start)

    def begin():
        from_peer(TWO)
        send(TWO, GU_1, DOWN_1, GU_2, DOWN_2, GU_3, GU_4)
        forward_x(ONE, GU_3[:1])

    def ready_gu(l, k, j, *pieces):
        landed(l, *pieces)
        stage_gu(l, k, j, start)

    def ready_d(l, k, j, *pieces):
        landed(l, *pieces)
        stage_d(l, k, j, start)

    def ready(l, k, j, *pieces):
        landed(l, *pieces)
        stage(l, k, j, start)

    def later(f, *args):
        return lambda: f(*args)

    def pass_later(*args):
        def go():
            for f, *rest in args:
                f(*rest)

        return go

    X, Y = forward_x, forward_y

    @pl.loop(0, 4)
    def _(k):
        stage(ONE, k, near_first(k), drain)

        @pl.loop(0, T // TM)
        def _(t):
            forward(k, t)
            duties(
                t, k,
                (FIRST, FIRST, begin),
                (SECOND, FIRST, pass_later((X, ONE, GU_3[1:]), (Y, ONE, GU_2))),
                (THIRD, FIRST, later(ready, ONE, SECOND, near_first(SECOND), GU_2)),
                (FIRST, SECOND, pass_later((X, ONE, DOWN_1), (Y, ONE, GU_3))),
                (SECOND, SECOND, pass_later((X, ONE, GU_4[:1]))),
                (SECOND, SECOND, later(ready_gu, ONE, THIRD, near_first(THIRD), GU_3)),
                (THIRD, SECOND, pass_later((X, ONE, GU_4[1:]), (Y, ONE, DOWN_1))),
                (LAST, SECOND, later(ready_d, ONE, THIRD, near_first(THIRD), DOWN_1)),
                (FIRST, THIRD, pass_later((X, ONE, DOWN_2), (Y, ONE, GU_4))),
                (SECOND, THIRD, later(ready_gu, ONE, LAST, near_first(LAST), GU_4)),
                (THIRD, THIRD, pass_later((X, TWO, GU_1[:1]))),
                (LAST, THIRD, pass_later((X, TWO, GU_1[1:]), (Y, ONE, DOWN_2))),
                (LAST, THIRD, later(ready_d, ONE, LAST, near_first(LAST), DOWN_2)),
                (FIRST, LAST, pass_later((X, TWO, DOWN_1), (Y, TWO, GU_1))),
                (SECOND, LAST, later(ready_gu, TWO, FIRST, far_first(FIRST), GU_1)),
                (THIRD, LAST, pass_later((X, TWO, GU_2[:1]))),
                (LAST, LAST, pass_later((X, TWO, GU_2[1:]), (Y, TWO, DOWN_1))),
            )

    load_dy.wait()
    for n in (THIRD, LAST):
        saving(near_first(LAST), n, drain)

    @pl.loop(0, T // 256)
    def _(t):
        r = pl.ds(pl.multiple_of(t * 256, 256), 256)
        wide = (h[r, :].astype(f32) + acc[r, :].astype(bf16).astype(f32)).astype(bf16)
        h[r, :] = wide
        wide = wide.astype(f32)
        a1[r, :] = (wide * scale_of(wide)).astype(bf16)
        acc[r, :] = jnp.zeros((256, D), f32)

        @pl.when(t == SECOND)
        def _():
            ready_d(TWO, FIRST, far_first(FIRST), DOWN_1)


    def gu_copies(l, k, j, act):
        act(remote(sg.at[3], rd3.at[k % 2], d_s.at[0], d_r3.at[k % 2], at_p))
        act(remote(sg.at[2], rd2_hbm.at[l, j], d_s.at[1], d_r2.at[l, j], at_p))
        act(pltpu.make_async_copy(sg.at[0], p0_hbm.at[l, j], keep.at[0]))

    def far_copy(q):
        return remote(sd.at[q, rows(DH * (1 - c), DH), :], rd3d.at[q], dd_s.at[0, q], d_r3d.at[q], at_p)

    def near_copy(l, q, act):
        @pl.when(c != q)
        def _():
            act(remote(sd.at[q], rd_d.at[l], dd_s.at[1, q], d_rd.at[l], at_p))

        @pl.when(c == q)
        def _():
            act(pltpu.make_async_copy(sd.at[q], own_d.at[l], keep.at[1]))

    def round_gu():
        for r, dest in ((3, iq), (1, ix), (2, ip), (0, i)):
            for m in range(2):
                sg[r, RB * m : RB * (m + 1), :] = acc_gu[rows(RB * dest, RB), m * C : (m + 1) * C].astype(bf16)
        clear(acc_gu, 128)

    def round_d(q):
        sd[q] = acc_d[...].astype(bf16)
        clear(acc_d, 128)

    def x_copy(l, k, j):
        return remote(sx.at[k], rx_hbm.at[l, j], x_s.at[k], x_r.at[l, j], at_x)

    def xd_copy(l, q):
        return remote(sxd.at[l, q], rx_d.at[l, rows(DH * c, DH), :], xd_s.at[l, q], xd_r.at[l, c], (y, 2 * (1 - xx) + q))

    def gu_across(l, k, j):
        remote(sg.at[3], rd3.at[k % 2], d_s.at[0], d_r3.at[k % 2], at_p).wait_recv()
        if l == ONE:
            x_copy(l, k, j).wait_send()
        sx[k] = (sg[1].astype(f32) + rd3[k % 2].astype(f32)).astype(bf16)
        x_copy(l, k, j).start()
        gu_copies(l, k, j, drain)

    def d_across(l, q):
        far_copy(q).wait_recv()
        sxd[l, q] = (sd[q, rows(DH * c, DH), :].astype(f32) + rd3d[q].astype(f32)).astype(bf16)
        xd_copy(l, q).start()
        drain(far_copy(q))

    def bring(n, part, act):
        act(pltpu.make_async_copy(part, h.at[n * 384 : (n + 1) * 384, :], fsem.at[n]))

    def put(n, dst, act):
        act(pltpu.make_async_copy(h.at[1152 + RB * n : 1152 + RB * (n + 1), :], dst, fout.at[n]))

    def add_up(parts, puts):
        for n, part in enumerate(parts):
            bring(n, part, drain)
        for r in range(0, 384, 128):
            g = h[r : r + 128, :].astype(f32) + h[384 + r : 512 + r, :].astype(f32) + h[768 + r : 896 + r, :].astype(f32)
            g = g.astype(bf16)
            h[1152 + r : 1280 + r, :] = g
            g = g.astype(f32)
            ssq[...] += jnp.sum((g * g).reshape(16, 8, D), axis=0)
        for n, dst in enumerate(puts):
            put(n, dst, start)

    def put_done():
        for n in range(2):
            put(n, gg_hbm.at[0, :, 0:C], drain)

    def gu_parts(l, k):
        j = near_first(k)
        return [p0_hbm.at[l, j], rd2_hbm.at[l, j], rx_hbm.at[l, j]]

    def bring_gu(l, k):
        j = near_first(k)
        parts = gu_parts(l, k)
        remote(sg.at[2], parts[1], d_s.at[1], d_r2.at[l, j], at_p).wait_recv()
        bring(0, parts[0], start)
        bring(1, parts[1], start)
        remote(sx.at[0], parts[2], x_s.at[0], x_r.at[l, j], at_x).wait_recv()
        bring(2, parts[2], start)

    def add_gu(l, k):
        j = near_first(k)
        add_up(gu_parts(l, k), [gg_hbm.at[l, :, cols(j)], gu_hbm.at[l, :, cols(j)]])

    def d_parts(l, half):
        r = rows(half * DH, DH)
        return [own_d.at[l, r, :], rd_d.at[l, r, :], rx_d.at[l, r, :]]

    def bring_d(l, half):
        parts = d_parts(l, half)
        remote(sxd.at[0, 0], parts[2], xd_s.at[0, 0], xd_r.at[l, half], at_x).wait_recv()
        for n, part in enumerate(parts):
            bring(n, part, start)

    def add_d(l, half):
        add_up(d_parts(l, half), [gd_hbm.at[l, rows(half * DH + RB * n, RB), :] for n in range(2)])

    def other_core_d(l):
        remote(sd.at[0], rd_d.at[l], dd_s.at[1, 0], d_rd.at[l], at_p).wait_recv()

    def through(gate, up, dact):
        dact = dact.astype(bf16).astype(f32)
        sig = jax.nn.sigmoid(gate)
        silu = gate * sig
        dgu_s[:, C:] = (dact * silu).astype(bf16)
        dgu_s[:, :C] = (dact * up * (sig + silu * (1.0 - sig))).astype(bf16)
        return (silu * up).astype(bf16)

    def backward_2(k, t):
        r, s = tile(t), k % 2
        gu = dot(a1[r, :], w_gu[s])
        act_s[...] = through(gu[:, :C], gu[:, C:], dot(do[r, :], w_d[s], NT))
        acc[r, :] += dot(dgu_s[...], w_gu[s], NT)
        acc_gu[...] += dot(a1[r, :], dgu_s[...], TN)
        acc_d[...] += dot(act_s[...], do[r, :], TN)

    def saved(j, t):
        return pltpu.make_async_copy(up_hbm.at[j, tile(t), :], up_s.at[t % 2], back.at[t % 2])

    def backward_1(k, t):
        r, s = tile(t), t % 2
        saved(far_first(k), t).wait()

        @pl.when(t < LAST)
        def _():
            saved(far_first(k), t + 1).start()

        @pl.when((t == LAST) & (k < LAST))
        def _():
            saved(far_first(k + 1), FIRST).start()

        through(up_s[s, :, :C], up_s[s, :, C:], dot(do[r, :], w_d[k % 2], NT))
        acc_gu[...] += dot(a0[r, :], dgu_s[...], TN)

    @pl.loop(0, 4)
    def _(k):
        stage(TWO, k, far_first(k), drain)

        @pl.loop(0, T // TM)
        def _(t):
            backward_2(k, t)

            def sums():
                @pl.when(k > FIRST)
                def _():
                    gu_across(TWO, k - 1, far_first(k - 1))

                @pl.when((k == SECOND) | (k == THIRD))
                def _():
                    d_across(TWO, k - 1)

            duties(
                t, k,
                (FIRST, None, sums),
                (FIRST, FIRST, pass_later((X, TWO, DOWN_2), (Y, TWO, GU_2))),
                (SECOND, FIRST, pass_later((X, TWO, GU_3), (Y, TWO, DOWN_2))),
                (THIRD, FIRST, pass_later((X, TWO, GU_4))),
                (THIRD, FIRST, later(ready, TWO, SECOND, far_first(SECOND), GU_2, DOWN_2)),
                (LAST, FIRST, pass_later((Y, TWO, GU_3))),
                (FIRST, SECOND, pass_later((Y, TWO, GU_4))),
                (THIRD, SECOND, later(ready, TWO, THIRD, far_first(THIRD), GU_3)),
                (THIRD, THIRD, later(ready, TWO, LAST, far_first(LAST), GU_4)),
                (FIRST, LAST, later(near_copy, TWO, 0, drain)),
                (THIRD, LAST, later(stage_d, ONE, FIRST, far_first(FIRST), start)),
            )

        round_gu()
        round_d(k % 2)
        gu_copies(TWO, k, far_first(k), start)

        @pl.when(k < THIRD)
        def _():
            far_copy(k).start()

        @pl.when(k >= THIRD)
        def _():
            near_copy(TWO, k - 2, start)

    def product(j, to):
        return pltpu.make_async_copy(act_hbm.at[j], to, ld.at[0])

    product(far_first(FIRST), a1).start()
    saved(far_first(FIRST), FIRST).start()

    @pl.loop(0, T // 256)
    def _(t):
        r = pl.ds(pl.multiple_of(t * 256, 256), 256)
        wide = h[r, :].astype(f32)
        scale = scale_of(wide)
        da = acc[r, :].astype(bf16).astype(f32)
        mix = jnp.sum(da * wide, -1, keepdims=True) * (scale * scale * scale / D)
        down = (da * scale - wide * mix).astype(bf16)
        do[r, :] = (do[r, :].astype(f32) + down.astype(f32)).astype(bf16)

    gu_across(TWO, LAST, far_first(LAST))

    def wide_halves(ref, to, sems):
        for l in range(L):
            for half in range(2):
                r = (2 * l + half) * RB
                yield pltpu.make_async_copy(ref.at[l, :, half * 2 * C : (half + 1) * 2 * C], to(l, half, r), sems.at[2 * l + half])

    def early_loads():
        for m, ref in enumerate((wg, wu)):
            yield from wide_halves(ref, lambda l, half, r: w_gu.at[m, r : r + RB, :], early.at[m])
        for l in range(L):
            yield pltpu.make_async_copy(m_down.at[l], acc.at[l * C : (l + 1) * C, :], early.at[2, l])

    def late_loads():
        yield from wide_halves(m_gate, lambda l, half, r: acc_gu.at[r : r + RB, :], late.at[0])
        yield from wide_halves(m_up, lambda l, half, r: up_s.at[l, half * RB : (half + 1) * RB, :], late.at[1])
        for l in range(L):
            yield pltpu.make_async_copy(wd.at[l], w_d.at[l], late.at[2, l])

    for load in early_loads():
        load.start()

    def down_grad(k, of, then, then_of):
        product(far_first(k), of).wait()
        if then is not None:
            product(far_first(then), then_of).start()

        @pl.loop(0, T // TM)
        def _(t):
            acc_d[...] += dot(of[tile(t), :], do[tile(t), :], TN)

    down_grad(FIRST, a1, SECOND, h)
    round_d(0)
    far_copy(0).start()
    down_grad(SECOND, h, THIRD, a1)
    near_copy(TWO, 1, drain)
    d_across(ONE, 0)
    round_d(1)
    far_copy(1).start()
    down_grad(THIRD, a1, LAST, h)
    d_across(ONE, 1)
    round_d(0)
    near_copy(ONE, 0, start)
    down_grad(LAST, h, None, None)
    near_copy(ONE, 0, drain)
    round_d(1)
    near_copy(ONE, 1, start)

    @pl.loop(0, 4)
    def _(k):
        stage_d(ONE, k, far_first(k), drain)

        @pl.loop(0, T // TM)
        def _(t):
            backward_1(k, t)

            def fetch():
                @pl.when(k == FIRST)
                def _():
                    near_copy(ONE, 1, drain)
                    other_core_d(TWO)

                @pl.when((k == SECOND) | (k == THIRD))
                def _():
                    add_d(TWO, k - 1)

                @pl.when(k > FIRST)
                def _():
                    put_done()

                bring_gu(TWO, k)

            def sums():
                @pl.when(k > FIRST)
                def _():
                    gu_across(ONE, k - 1, far_first(k - 1))

                @pl.when(k < LAST)
                def _():
                    stage_d(ONE, k + 1, far_first(k + 1), start)

            def fetch_d():
                @pl.when(k < THIRD)
                def _():
                    put_done()
                    bring_d(TWO, k)

            duties(
                t, k,
                (FIRST, None, fetch),
                (SECOND, None, sums),
                (THIRD, None, later(add_gu, TWO, k)),
                (LAST, None, fetch_d),
            )

        round_gu()
        gu_copies(ONE, k, far_first(k), start)

    for load in late_loads():
        load.start()
    gu_across(ONE, LAST, far_first(LAST))
    other_core_d(ONE)

    @pl.loop(0, 2)
    def _(half):
        put_done()
        bring_d(ONE, half)
        add_d(ONE, half)

    @pl.loop(0, 4)
    def _(k):
        put_done()
        bring_gu(ONE, k)
        add_gu(ONE, k)

    part = ssq[:, :128]
    for n in range(1, D // 128):
        part = part + ssq[:, n * 128 : (n + 1) * 128]
    ss_src[...] = part
    for l in range(L):
        for p in range(10):
            for which, (src, half, to) in enumerate(((ix, y, at_x), (ix, y, at_y), (ix, y, at_p), (ix, 1 - y, at_p))):
                if which == OVER_X:
                    send_x(l, p, drain)
                else:
                    r = mine(l, p, src, half)
                    remote(r, r, ag_s.at[l, p, which], ag_r.at[l, p, which], to).wait_send()
        for m in range(3):
            to_peer(l, m).wait_send()
        for q in range(2):
            xd_copy(l, q).wait_send()
    for k in range(4):
        x_copy(ONE, k, far_first(k)).wait_send()
    tells = [
        remote(ss_src, ss.at[i], ss_s.at[n], ss_r.at[i], to) for n, to in enumerate((at_x, at_p, at_q))
    ]
    for tell in tells:
        tell.start()
    for src in (ix, ip, iq):
        remote(ss_src, ss.at[src], ss_s.at[0], ss_r.at[src], at_x).wait_recv()
    for tell in tells:
        tell.wait_send()
    put_done()
    for load in (*early_loads(), *late_loads()):
        load.wait()
    ss[i] = part
    total = jnp.sum(ss[0] + ss[1] + ss[2] + ss[3])
    fac[...] = jnp.minimum(1.0, 0.5 * lax.rsqrt(jnp.full((8, 128), total / COUNT + 1e-30, f32)))


def gradients(x, dy, w, m):
    hbm = pl.BlockSpec(memory_space=pl.ANY)
    vmem = pl.BlockSpec(memory_space=pltpu.VMEM)
    out = lambda *shape: jax.ShapeDtypeStruct(shape, bf16)
    dma = lambda *shape: pltpu.SemaphoreType.DMA(shape)
    return pl.pallas_call(
        step_kernel,
        in_specs=[hbm] * 8,
        out_specs=[hbm] * 3 + [vmem] + [hbm] * 11 + [vmem] * 5,
        out_shape=[
            out(L, RB, FF), out(L, RB, FF), out(L, C, D), jax.ShapeDtypeStruct((8, 128), f32),
            out(L, D, FF), out(L, D, FF), out(L, FF, D),
            out(L, 4, 2 * RB, C), out(L, 4, 2 * RB, C), out(L, 4, 2 * RB, C),
            out(L, C, D), out(L, C, D), out(L, C, D),
            jax.ShapeDtypeStruct((4, T, 2 * C), f32), out(4, T, C),
            pltpu.VMEM((T, D), f32), pltpu.VMEM((D, 2 * C), f32), pltpu.VMEM((2, TM, 2 * C), f32),
            pltpu.VMEM((2, D, 2 * C), bf16), pltpu.VMEM((2, C, D), bf16),
        ],
        scratch_shapes=[
            pltpu.VMEM((T, D), bf16), pltpu.VMEM((T, D), bf16), pltpu.VMEM((T, D), bf16), pltpu.VMEM((T, D), bf16),
            pltpu.VMEM((C, D), f32),
            pltpu.VMEM((TM, C), bf16), pltpu.VMEM((TM, 2 * C), bf16),
            pltpu.VMEM((4, 2 * RB, C), bf16), pltpu.VMEM((2, C, D), bf16),
            pltpu.VMEM((2, 2 * RB, C), bf16), pltpu.VMEM((2, DH, D), bf16),
            pltpu.VMEM((4, 2 * RB, C), bf16), pltpu.VMEM((2, 2, DH, D), bf16),
            pltpu.VMEM((8, D), f32), pltpu.VMEM((4, 8, 128), f32), pltpu.VMEM((8, 128), f32),
            dma(L, 10, 4), dma(L, 10, 4), dma(L, 3), dma(L, 3), dma(2), dma(2, 7),
            dma(2), dma(2), dma(2, 2), dma(2), dma(L, 4), dma(L), dma(2), dma(4), dma(L, 4), dma(L, 2), dma(L, 2),
            dma(3), dma(2), dma(3), dma(4), dma(2, 2), dma(2), dma(3, 4), dma(3, 4),
        ],
        compiler_params=pltpu.CompilerParams(
            collective_id=0, has_side_effects=True, vmem_limit_bytes=MEGA * 2**20
        ),
        name="train_step",
    )(x, dy, *w, *m)


def adamw_kernel(*refs):
    fac, ins, outs = refs[0], refs[1:13], refs[13:]
    factor = fac[0:1, 0:1]
    for n in range(3):
        g, w, m, v = (ins[3 * which + n] for which in range(4))
        shape = g.shape[1:]
        grad = g[0].astype(f32) * factor
        new_m = 0.9 * m[...].reshape(shape) + 0.1 * grad
        new_v = 0.95 * v[0] + 0.05 * grad * grad
        wide = w[0].astype(f32)
        outs[n][0] = (wide - 0.02 * (new_m * lax.rsqrt(new_v + 1e-8) + 0.1 * wide)).astype(bf16)
        outs[3 + n][0] = new_m
        outs[6 + n][0] = new_v


def adamw(factor, g, v, m_down, m_gate, m_up, w_gu, w_d):
    n = 2
    rows, tall = RB // n, C // (2 * n)
    half = (rows, 2 * C)
    wide = pl.BlockSpec((1, *half), lambda t: (t // (2 * n), t % n, t // n % 2))
    down = pl.BlockSpec((1, tall, D), lambda t: (t // (2 * n), t % (2 * n), 0))
    w_at = lambda which: pl.BlockSpec((1, *half), lambda t: (which, t, 0))
    specs = [wide, wide, down]
    shapes = lambda dtype: [jax.ShapeDtypeStruct(a.shape, dtype) for a in v]
    return pl.pallas_call(
        adamw_kernel,
        grid=(2 * n * L,),
        in_specs=[pl.BlockSpec((8, 128), lambda t: (0, 0))]
        + specs
        + [w_at(0), w_at(1), down]
        + [
            pl.BlockSpec(half, lambda t: (t, 0)),
            pl.BlockSpec((1, *half), lambda t: (t // (2 * n), t % (2 * n), 0)),
            pl.BlockSpec((tall, D), lambda t: (t, 0)),
        ]
        + specs,
        out_specs=specs * 3,
        out_shape=shapes(bf16) + shapes(f32) + shapes(f32),
        compiler_params=pltpu.CompilerParams(vmem_limit_bytes=ADAMW * 2**20),
        name="adamw",
    )(factor, *g, *(pltpu.with_memory_space_constraint(a, pltpu.VMEM) for a in (w_gu, w_gu, w_d, m_gate, m_up, m_down)), *v)


def solution(mesh):
    def step(x, dy, *arrays):
        w, m, v = (arrays[n : n + 3] for n in (0, 3, 6))
        gg, gu, gd, factor, *rest = gradients(x[0], dy[0], w, m)
        return tuple(adamw(factor, (gg, gu, gd), v, *rest[-5:]))

    states, cut = P(("rep", "dp"), None, None), P(None, "dp", None)
    return jax.shard_map(
        step,
        mesh=mesh,
        in_specs=(states, states) + (cut,) * 9,
        out_specs=(P("rep", "dp", None),) * 9,
        check_vma=False,
    )
```

```python
import functools

import jax
import jax.numpy as jnp
from jax import lax
from jax.experimental import pallas as pl
from jax.experimental.pallas import tpu as pltpu
from jax.sharding import PartitionSpec as P

T, D, FF, L = 2048, 768, 3072, 2
C = 768
TM = 512
RB = D // 4
RH = RB // 2
DH = C // 2
DQ = C // 4
ADAMW = 40
MEGA = 40
COUNT = 3 * L * D * FF
FIRST, SECOND, THIRD, LAST = range(4)
OVER_X, OVER_Y, TO_CORE, Y_TO_CORE = range(4)
GU = [(n, n + 1) for n in range(0, 8, 2)]
GU_1, GU_2, GU_3, GU_4 = GU
DOWN_1, DOWN_2 = (8,), (9,)
ONE, TWO = range(L)
bf16, f32 = jnp.bfloat16, jnp.float32
NT = (((1,), (1,)), ((), ()))
TN = (((0,), (0,)), ((), ()))
MESH = pl.DeviceIdType.MESH


def dot(a, b, dims=(((1,), (0,)), ((), ()))):
    return lax.dot_general(a, b, dims, preferred_element_type=f32)


def scale_of(wide):
    return lax.rsqrt(jnp.mean(wide * wide, -1, keepdims=True) + 1e-6)


def step_kernel(
    x_hbm, dy_hbm, wg, wu, wd, m_gate, m_up, m_down,
    gg_hbm, gu_hbm, gd_hbm, fac, all_g, all_u, all_d, p0_hbm, rd2_hbm, rx_hbm, own_d, rd_d, rx_d, up_hbm, act_hbm,
    acc, acc_gu, up_s, w_gu, w_d,
    h, a0, a1, do, acc_d, act_s, dgu_s, sg, sd, rd3, rd3d, sx, sxd, ssq, ss, ss_src,
    ag_s, ag_r, pe_s, pe_r, ld, wsem, d_s, d_r3, dd_s, d_r3d, d_r2, d_rd, keep, x_s, x_r, xd_s, xd_r, fsem, fout, ss_s, ss_r, save, back, early, late,
):
    y, i = lax.axis_index("rep"), lax.axis_index("dp")
    xx, c = i // 2, i % 2
    ix, ip, iq = (1 - xx) * 2 + c, xx * 2 + 1 - c, (1 - xx) * 2 + 1 - c
    at_x, at_p, at_q, at_y = (y, ix), (y, ip), (y, iq), (1 - y, i)

    def remote(src, dst, send, recv, to):
        return pltpu.make_async_remote_copy(
            src_ref=src, dst_ref=dst, send_sem=send, recv_sem=recv, device_id=to, device_id_type=MESH
        )

    def near_first(k):
        return (2 * xx + k) % 4

    def far_first(k):
        return (2 * (1 - xx) + k) % 4

    def start(copy):
        copy.start()

    def drain(copy):
        copy.wait_send() if copy.is_remote else copy.wait()

    def duties(t, k, *work):
        for n in range(T // TM):
            here = [(m, f) for tile_n, m, f in work if tile_n == n]
            if here:

                @pl.when(t == n)
                def _():
                    for m, f in here:
                        if m is None:
                            f()
                        else:
                            pl.when(k == m)(f)

    def cols(j):
        return pl.ds(pl.multiple_of(j * C, C), C)

    def rows(start, size):
        return pl.ds(pl.multiple_of(start, 32), size)

    barrier = pltpu.get_barrier_semaphore()
    for other in (at_x, at_p, at_q, at_y):
        pl.semaphore_signal(barrier, inc=1, device_id=other, device_id_type=MESH)
    load_x = pltpu.make_async_copy(x_hbm, h, ld.at[0])
    load_dy = pltpu.make_async_copy(dy_hbm, do, ld.at[1])
    load_x.start()
    load_dy.start()
    pl.semaphore_wait(barrier, 4)

    def region(l, p, src, half, j):
        if p >= 8:
            return all_d.at[l, rows(C * (src // 2 * 2 + p - 8) + DH * half + DQ * (src % 2), DQ), :]
        return (all_g, all_u)[p % 2].at[l, rows(RB * src + RH * half, RH), cols(j)]

    def mine(l, p, src, half):
        return region(l, p, src, half, (near_first, far_first)[l](p // 2))

    def send_x(l, p, act):
        j = (far_first, near_first)[l](p // 2)
        there = region(l, p, i, y, j)

        def copy(src):
            return remote(src, there, ag_s.at[l, p, OVER_X], ag_r.at[l, p, OVER_X], at_x)

        if p < 8:
            act(copy((wg, wu)[p % 2].at[l, rows(RH * y, RH), cols(j)]))
        elif act is start:

            @pl.when(c == p - 8)
            def _():
                act(copy(wd.at[l, rows(DH * y + DQ * c, DQ), :]))

            @pl.when(c != p - 8)
            def _():
                act(copy(there))
        else:
            act(copy(there))

    def forward_x(l, *pieces):
        for p in sum(pieces, ()):
            r = mine(l, p, ix, y)
            remote(r, r, ag_s.at[l, p, OVER_X], ag_r.at[l, p, OVER_X], at_x).wait_recv()
            remote(r, r, ag_s.at[l, p, OVER_Y], ag_r.at[l, p, OVER_Y], at_y).start()
            remote(r, r, ag_s.at[l, p, TO_CORE], ag_r.at[l, p, TO_CORE], at_p).start()

    def forward_y(l, *pieces):
        for p in sum(pieces, ()):
            r = mine(l, p, ix, 1 - y)
            remote(r, r, ag_s.at[l, p, OVER_Y], ag_r.at[l, p, OVER_Y], at_y).wait_recv()
            remote(r, r, ag_s.at[l, p, Y_TO_CORE], ag_r.at[l, p, Y_TO_CORE], at_p).start()

    def landed(l, *pieces):
        for p in sum(pieces, ()):
            for which, half in ((TO_CORE, y), (Y_TO_CORE, 1 - y)):
                r = mine(l, p, iq, half)
                remote(r, r, ag_s.at[l, p, which], ag_r.at[l, p, which], at_p).wait_recv()

    def to_peer(l, m):
        src = (wg, wu, wd)[m].at[l]
        dst = (all_g.at[l, rows(RB * i, RB), :], all_u.at[l, rows(RB * i, RB), :], all_d.at[l, rows(C * i, C), :])[m]
        return remote(src, dst, pe_s.at[l, m], pe_r.at[l, m], at_p)

    def from_peer(l):
        for m in range(3):
            to_peer(l, m).wait_recv()

    def send(l, *pieces):
        for p in sum(pieces, ()):
            send_x(l, p, start)

    send(ONE, GU_1, GU_2, GU_3)
    for l in range(L):
        for m in range(3):
            to_peer(l, m).start()

    def stage_gu(l, k, j, act):
        slot = k % 2
        for m, (own, gathered) in enumerate(((wg, all_g), (wu, all_u))):
            for n, (src, row, size) in enumerate(
                (
                    (own.at[l, :, cols(j)], RB * i, RB),
                    (gathered.at[l, rows(RB * ip, RB), cols(j)], RB * ip, RB),
                    (gathered.at[l, rows(2 * RB * (1 - xx), 2 * RB), cols(j)], 2 * RB * (1 - xx), 2 * RB),
                )
            ):
                copy = pltpu.make_async_copy(
                    src, w_gu.at[slot, rows(row, size), m * C : (m + 1) * C], wsem.at[slot, 3 * m + n]
                )
                act(copy)

    def stage_d(l, k, j, act):
        slot = k % 2
        theirs = pltpu.make_async_copy(all_d.at[l, rows(C * j, C), :], w_d.at[slot], wsem.at[slot, 6])
        if act is start:

            @pl.when(j == i)
            def _():
                pltpu.make_async_copy(wd.at[l], w_d.at[slot], wsem.at[slot, 6]).start()

            @pl.when(j != i)
            def _():
                theirs.start()
        else:
            act(theirs)

    def stage(l, k, j, act):
        stage_gu(l, k, j, act)
        stage_d(l, k, j, act)

    def tile(t):
        return pl.ds(pl.multiple_of(t * TM, TM), TM)

    def clear(ref, size):
        n = ref.shape[0] // size

        @pl.loop(0, n)
        def _(t):
            ref[pl.ds(pl.multiple_of(t * size, size), size), :] = jnp.zeros((size, ref.shape[1]), ref.dtype)

    clear(acc, 256)
    clear(acc_gu, 128)
    clear(acc_d, 128)
    ssq[...] = jnp.zeros_like(ssq)
    load_x.wait()

    @pl.loop(0, T // 256)
    def _(t):
        r = pl.ds(pl.multiple_of(t * 256, 256), 256)
        wide = h[r, :].astype(f32)
        a0[r, :] = (wide * scale_of(wide)).astype(bf16)

    def saving(j, t, act):
        s = t % 2
        act(pltpu.make_async_copy(up_s.at[s], up_hbm.at[j, tile(t), :], save.at[0, s]))
        act(pltpu.make_async_copy(dgu_s.at[:, cols(s)], act_hbm.at[j, tile(t), :], save.at[1, s]))

    def forward(k, t):
        r, s = tile(t), t % 2

        @pl.when((k > 0) | (t > 1))
        def _():
            saving(near_first(k), t, drain)

        gu = dot(a0[r, :], w_gu[k % 2])
        up_s[s] = gu
        gate, up = gu[:, :C], gu[:, C:]
        act = (gate * jax.nn.sigmoid(gate) * up).astype(bf16)
        dgu_s[:, cols(s)] = act
        saving(near_first(k), t, start)
        acc[r, :] += dot(act, w_d[k % 2])

    forward_x(ONE, GU_1)
    from_peer(ONE)
    send(ONE, DOWN_1, GU_4, DOWN_2)
    forward_x(ONE, GU_2)
    forward_y(ONE, GU_1)
    landed(ONE, GU_1)
    stage(ONE, FIRST, near_first(FIRST), start)

    def begin():
        from_peer(TWO)
        send(TWO, GU_1, DOWN_1, GU_2, DOWN_2, GU_3, GU_4)
        forward_x(ONE, GU_3[:1])

    def ready_gu(l, k, j, *pieces):
        landed(l, *pieces)
        stage_gu(l, k, j, start)

    def ready_d(l, k, j, *pieces):
        landed(l, *pieces)
        stage_d(l, k, j, start)

    def ready(l, k, j, *pieces):
        landed(l, *pieces)
        stage(l, k, j, start)

    def later(f, *args):
        return lambda: f(*args)

    def pass_later(*args):
        def go():
            for f, *rest in args:
                f(*rest)

        return go

    X, Y = forward_x, forward_y

    @pl.loop(0, 4)
    def _(k):
        stage(ONE, k, near_first(k), drain)

        @pl.when(k == THIRD)
        def _():
            forward_x(ONE, DOWN_2)

        @pl.loop(0, T // TM)
        def _(t):
            forward(k, t)
            duties(
                t, k,
                (FIRST, FIRST, begin),
                (SECOND, FIRST, pass_later((X, ONE, GU_3[1:]), (Y, ONE, GU_2))),
                (THIRD, FIRST, later(ready, ONE, SECOND, near_first(SECOND), GU_2)),
                (FIRST, SECOND, pass_later((X, ONE, DOWN_1), (Y, ONE, GU_3))),
                (SECOND, SECOND, pass_later((X, ONE, GU_4[:1]))),
                (SECOND, SECOND, later(ready_gu, ONE, THIRD, near_first(THIRD), GU_3)),
                (THIRD, SECOND, pass_later((X, ONE, GU_4[1:]), (Y, ONE, DOWN_1))),
                (LAST, SECOND, later(ready_d, ONE, THIRD, near_first(THIRD), DOWN_1)),
                (FIRST, THIRD, pass_later((Y, ONE, GU_4))),
                (SECOND, THIRD, later(ready_gu, ONE, LAST, near_first(LAST), GU_4)),
                (THIRD, THIRD, pass_later((X, TWO, GU_1), (Y, ONE, DOWN_2))),
                (LAST, THIRD, later(ready_d, ONE, LAST, near_first(LAST), DOWN_2)),
                (FIRST, LAST, pass_later((X, TWO, DOWN_1), (Y, TWO, GU_1))),
                (SECOND, LAST, later(ready_gu, TWO, FIRST, far_first(FIRST), GU_1)),
                (THIRD, LAST, pass_later((X, TWO, GU_2[:1]))),
                (LAST, LAST, pass_later((X, TWO, GU_2[1:]), (Y, TWO, DOWN_1))),
            )

    load_dy.wait()
    for n in (THIRD, LAST):
        saving(near_first(LAST), n, drain)

    @pl.loop(0, T // 256)
    def _(t):
        r = pl.ds(pl.multiple_of(t * 256, 256), 256)
        wide = (h[r, :].astype(f32) + acc[r, :].astype(bf16).astype(f32)).astype(bf16)
        h[r, :] = wide
        wide = wide.astype(f32)
        a1[r, :] = (wide * scale_of(wide)).astype(bf16)
        acc[r, :] = jnp.zeros((256, D), f32)

        @pl.when(t == LAST)
        def _():
            ready_d(TWO, FIRST, far_first(FIRST), DOWN_1)


    def gu_copies(l, k, j, act):
        act(remote(sg.at[3], rd3.at[k % 2], d_s.at[0], d_r3.at[k % 2], at_p))
        act(remote(sg.at[2], rd2_hbm.at[l, j], d_s.at[1], d_r2.at[l, j], at_p))
        act(pltpu.make_async_copy(sg.at[0], p0_hbm.at[l, j], keep.at[0]))

    def far_copy(q):
        return remote(sd.at[q, rows(DH * (1 - c), DH), :], rd3d.at[q], dd_s.at[0, q], d_r3d.at[q], at_p)

    def near_copy(l, q, act):
        @pl.when(c != q)
        def _():
            act(remote(sd.at[q], rd_d.at[l], dd_s.at[1, q], d_rd.at[l], at_p))

        @pl.when(c == q)
        def _():
            act(pltpu.make_async_copy(sd.at[q], own_d.at[l], keep.at[1]))

    def round_gu():
        for r, dest in ((3, iq), (1, ix), (2, ip), (0, i)):
            for m in range(2):
                sg[r, RB * m : RB * (m + 1), :] = acc_gu[rows(RB * dest, RB), m * C : (m + 1) * C].astype(bf16)
        clear(acc_gu, 128)

    def round_d(q):
        sd[q] = acc_d[...].astype(bf16)
        clear(acc_d, 128)

    def x_copy(l, k, j):
        return remote(sx.at[k], rx_hbm.at[l, j], x_s.at[k], x_r.at[l, j], at_x)

    def xd_copy(l, q):
        return remote(sxd.at[l, q], rx_d.at[l, rows(DH * c, DH), :], xd_s.at[l, q], xd_r.at[l, c], (y, 2 * (1 - xx) + q))

    def gu_across(l, k, j):
        remote(sg.at[3], rd3.at[k % 2], d_s.at[0], d_r3.at[k % 2], at_p).wait_recv()
        if l == ONE:
            x_copy(l, k, j).wait_send()
        sx[k] = (sg[1].astype(f32) + rd3[k % 2].astype(f32)).astype(bf16)
        x_copy(l, k, j).start()
        gu_copies(l, k, j, drain)

    def d_across(l, q):
        far_copy(q).wait_recv()
        sxd[l, q] = (sd[q, rows(DH * c, DH), :].astype(f32) + rd3d[q].astype(f32)).astype(bf16)
        xd_copy(l, q).start()
        drain(far_copy(q))

    def bring(n, part, act):
        act(pltpu.make_async_copy(part, h.at[n * 384 : (n + 1) * 384, :], fsem.at[n]))

    def put(n, dst, act):
        act(pltpu.make_async_copy(h.at[1152 + RB * n : 1152 + RB * (n + 1), :], dst, fout.at[n]))

    def add_up(parts, puts):
        for n, part in enumerate(parts):
            bring(n, part, drain)
        for r in range(0, 384, 128):
            g = h[r : r + 128, :].astype(f32) + h[384 + r : 512 + r, :].astype(f32) + h[768 + r : 896 + r, :].astype(f32)
            g = g.astype(bf16)
            h[1152 + r : 1280 + r, :] = g
            g = g.astype(f32)
            ssq[...] += jnp.sum((g * g).reshape(16, 8, D), axis=0)
        for n, dst in enumerate(puts):
            put(n, dst, start)

    def put_done():
        for n in range(2):
            put(n, gg_hbm.at[0, :, 0:C], drain)

    def gu_parts(l, k):
        j = near_first(k)
        return [p0_hbm.at[l, j], rd2_hbm.at[l, j], rx_hbm.at[l, j]]

    def bring_gu(l, k):
        j = near_first(k)
        parts = gu_parts(l, k)
        remote(sg.at[2], parts[1], d_s.at[1], d_r2.at[l, j], at_p).wait_recv()
        bring(0, parts[0], start)
        bring(1, parts[1], start)
        remote(sx.at[0], parts[2], x_s.at[0], x_r.at[l, j], at_x).wait_recv()
        bring(2, parts[2], start)

    def add_gu(l, k):
        j = near_first(k)
        add_up(gu_parts(l, k), [gg_hbm.at[l, :, cols(j)], gu_hbm.at[l, :, cols(j)]])

    def d_parts(l, half):
        r = rows(half * DH, DH)
        return [own_d.at[l, r, :], rd_d.at[l, r, :], rx_d.at[l, r, :]]

    def bring_d(l, half):
        parts = d_parts(l, half)
        remote(sxd.at[0, 0], parts[2], xd_s.at[0, 0], xd_r.at[l, half], at_x).wait_recv()
        for n, part in enumerate(parts):
            bring(n, part, start)

    def add_d(l, half):
        add_up(d_parts(l, half), [gd_hbm.at[l, rows(half * DH + RB * n, RB), :] for n in range(2)])

    def other_core_d(l):
        remote(sd.at[0], rd_d.at[l], dd_s.at[1, 0], d_rd.at[l], at_p).wait_recv()

    def through(gate, up, dact):
        dact = dact.astype(bf16).astype(f32)
        sig = jax.nn.sigmoid(gate)
        silu = gate * sig
        dgu_s[:, C:] = (dact * silu).astype(bf16)
        dgu_s[:, :C] = (dact * up * (sig + silu * (1.0 - sig))).astype(bf16)
        return (silu * up).astype(bf16)

    def backward_2(k, t):
        r, s = tile(t), k % 2
        gu = dot(a1[r, :], w_gu[s])
        act_s[...] = through(gu[:, :C], gu[:, C:], dot(do[r, :], w_d[s], NT))
        acc[r, :] += dot(dgu_s[...], w_gu[s], NT)
        acc_gu[...] += dot(a1[r, :], dgu_s[...], TN)
        acc_d[...] += dot(act_s[...], do[r, :], TN)

    def saved(j, t):
        return pltpu.make_async_copy(up_hbm.at[j, tile(t), :], up_s.at[t % 2], back.at[t % 2])

    def backward_1(k, t):
        r, s = tile(t), t % 2
        saved(far_first(k), t).wait()

        @pl.when(t < LAST)
        def _():
            saved(far_first(k), t + 1).start()

        @pl.when((t == LAST) & (k < LAST))
        def _():
            saved(far_first(k + 1), FIRST).start()

        through(up_s[s, :, :C], up_s[s, :, C:], dot(do[r, :], w_d[k % 2], NT))
        acc_gu[...] += dot(a0[r, :], dgu_s[...], TN)

    @pl.loop(0, 4)
    def _(k):
        stage(TWO, k, far_first(k), drain)

        @pl.loop(0, T // TM)
        def _(t):
            backward_2(k, t)

            def sums():
                @pl.when(k > FIRST)
                def _():
                    gu_across(TWO, k - 1, far_first(k - 1))

                @pl.when((k == SECOND) | (k == THIRD))
                def _():
                    d_across(TWO, k - 1)

            duties(
                t, k,
                (FIRST, None, sums),
                (FIRST, FIRST, pass_later((X, TWO, DOWN_2), (Y, TWO, GU_2))),
                (SECOND, FIRST, pass_later((X, TWO, GU_3), (Y, TWO, DOWN_2))),
                (THIRD, FIRST, pass_later((X, TWO, GU_4))),
                (THIRD, FIRST, later(ready, TWO, SECOND, far_first(SECOND), GU_2, DOWN_2)),
                (LAST, FIRST, pass_later((Y, TWO, GU_3))),
                (FIRST, SECOND, pass_later((Y, TWO, GU_4))),
                (THIRD, SECOND, later(ready, TWO, THIRD, far_first(THIRD), GU_3)),
                (THIRD, THIRD, later(ready, TWO, LAST, far_first(LAST), GU_4)),
                (FIRST, LAST, later(near_copy, TWO, 0, drain)),
                (THIRD, LAST, later(stage_d, ONE, FIRST, far_first(FIRST), start)),
            )

        round_gu()
        round_d(k % 2)
        gu_copies(TWO, k, far_first(k), start)

        @pl.when(k < THIRD)
        def _():
            far_copy(k).start()

        @pl.when(k >= THIRD)
        def _():
            near_copy(TWO, k - 2, start)

    def product(j, to):
        return pltpu.make_async_copy(act_hbm.at[j], to, ld.at[0])

    product(far_first(FIRST), a1).start()
    saved(far_first(FIRST), FIRST).start()

    @pl.loop(0, T // 256)
    def _(t):
        r = pl.ds(pl.multiple_of(t * 256, 256), 256)
        wide = h[r, :].astype(f32)
        scale = scale_of(wide)
        da = acc[r, :].astype(bf16).astype(f32)
        mix = jnp.sum(da * wide, -1, keepdims=True) * (scale * scale * scale / D)
        down = (da * scale - wide * mix).astype(bf16)
        do[r, :] = (do[r, :].astype(f32) + down.astype(f32)).astype(bf16)

    gu_across(TWO, LAST, far_first(LAST))

    def wide_halves(ref, to, sems):
        for l in range(L):
            for half in range(2):
                r = (2 * l + half) * RB
                yield pltpu.make_async_copy(ref.at[l, :, half * 2 * C : (half + 1) * 2 * C], to(l, half, r), sems.at[2 * l + half])

    def early_loads():
        for m, ref in enumerate((wg, wu)):
            yield from wide_halves(ref, lambda l, half, r: w_gu.at[m, r : r + RB, :], early.at[m])
        for l in range(L):
            yield pltpu.make_async_copy(m_down.at[l], acc.at[l * C : (l + 1) * C, :], early.at[2, l])

    def late_loads():
        yield from wide_halves(m_gate, lambda l, half, r: acc_gu.at[r : r + RB, :], late.at[0])
        yield from wide_halves(m_up, lambda l, half, r: up_s.at[l, half * RB : (half + 1) * RB, :], late.at[1])
        for l in range(L):
            yield pltpu.make_async_copy(wd.at[l], w_d.at[l], late.at[2, l])

    for load in early_loads():
        load.start()

    def down_grad(k, of, then, then_of):
        product(far_first(k), of).wait()
        if then is not None:
            product(far_first(then), then_of).start()

        @pl.loop(0, T // TM)
        def _(t):
            acc_d[...] += dot(of[tile(t), :], do[tile(t), :], TN)

    down_grad(FIRST, a1, SECOND, h)
    round_d(0)
    far_copy(0).start()
    down_grad(SECOND, h, THIRD, a1)
    near_copy(TWO, 1, drain)
    d_across(ONE, 0)
    round_d(1)
    far_copy(1).start()
    down_grad(THIRD, a1, LAST, h)
    d_across(ONE, 1)
    round_d(0)
    near_copy(ONE, 0, start)
    down_grad(LAST, h, None, None)
    near_copy(ONE, 0, drain)
    round_d(1)
    near_copy(ONE, 1, start)

    @pl.loop(0, 4)
    def _(k):
        stage_d(ONE, k, far_first(k), drain)

        @pl.loop(0, T // TM)
        def _(t):
            backward_1(k, t)

            def fetch():
                @pl.when(k == FIRST)
                def _():
                    near_copy(ONE, 1, drain)
                    other_core_d(TWO)

                @pl.when((k == SECOND) | (k == THIRD))
                def _():
                    add_d(TWO, k - 1)

                @pl.when(k > FIRST)
                def _():
                    put_done()

                bring_gu(TWO, k)

            def sums():
                @pl.when(k > FIRST)
                def _():
                    gu_across(ONE, k - 1, far_first(k - 1))

                @pl.when(k < LAST)
                def _():
                    stage_d(ONE, k + 1, far_first(k + 1), start)

            def fetch_d():
                @pl.when(k < THIRD)
                def _():
                    put_done()
                    bring_d(TWO, k)

            duties(
                t, k,
                (FIRST, None, fetch),
                (SECOND, None, sums),
                (THIRD, None, later(add_gu, TWO, k)),
                (LAST, None, fetch_d),
            )

        round_gu()
        gu_copies(ONE, k, far_first(k), start)

    for load in late_loads():
        load.start()
    gu_across(ONE, LAST, far_first(LAST))
    for l in range(L):
        for p in range(10):
            for which, (src, half, to) in enumerate(((ix, y, at_x), (ix, y, at_y), (ix, y, at_p), (ix, 1 - y, at_p))):
                if which == OVER_X:
                    send_x(l, p, drain)
                else:
                    r = mine(l, p, src, half)
                    remote(r, r, ag_s.at[l, p, which], ag_r.at[l, p, which], to).wait_send()
        for m in range(3):
            to_peer(l, m).wait_send()
        for q in range(2):
            xd_copy(l, q).wait_send()
    for load in (*early_loads(), *late_loads()):
        load.wait()
    other_core_d(ONE)

    @pl.loop(0, 2)
    def _(half):
        put_done()
        bring_d(ONE, half)
        add_d(ONE, half)

    @pl.loop(0, 4)
    def _(k):
        put_done()
        bring_gu(ONE, k)
        add_gu(ONE, k)

    part = ssq[:, :128]
    for n in range(1, D // 128):
        part = part + ssq[:, n * 128 : (n + 1) * 128]
    ss_src[...] = part
    for k in range(4):
        x_copy(ONE, k, far_first(k)).wait_send()
    tells = [
        remote(ss_src, ss.at[i], ss_s.at[n], ss_r.at[i], to) for n, to in enumerate((at_x, at_p, at_q))
    ]
    for tell in tells:
        tell.start()
    for src in (ix, ip, iq):
        remote(ss_src, ss.at[src], ss_s.at[0], ss_r.at[src], at_x).wait_recv()
    for tell in tells:
        tell.wait_send()
    put_done()
    ss[i] = part
    total = jnp.sum(ss[0] + ss[1] + ss[2] + ss[3])
    fac[...] = jnp.minimum(1.0, 0.5 * lax.rsqrt(jnp.full((8, 128), total / COUNT + 1e-30, f32)))


def gradients(x, dy, w, m):
    hbm = pl.BlockSpec(memory_space=pl.ANY)
    vmem = pl.BlockSpec(memory_space=pltpu.VMEM)
    out = lambda *shape: jax.ShapeDtypeStruct(shape, bf16)
    dma = lambda *shape: pltpu.SemaphoreType.DMA(shape)
    return pl.pallas_call(
        step_kernel,
        in_specs=[hbm] * 8,
        out_specs=[hbm] * 3 + [vmem] + [hbm] * 11 + [vmem] * 5,
        out_shape=[
            out(L, RB, FF), out(L, RB, FF), out(L, C, D), jax.ShapeDtypeStruct((8, 128), f32),
            out(L, D, FF), out(L, D, FF), out(L, FF, D),
            out(L, 4, 2 * RB, C), out(L, 4, 2 * RB, C), out(L, 4, 2 * RB, C),
            out(L, C, D), out(L, C, D), out(L, C, D),
            jax.ShapeDtypeStruct((4, T, 2 * C), f32), out(4, T, C),
            pltpu.VMEM((T, D), f32), pltpu.VMEM((D, 2 * C), f32), pltpu.VMEM((2, TM, 2 * C), f32),
            pltpu.VMEM((2, D, 2 * C), bf16), pltpu.VMEM((2, C, D), bf16),
        ],
        scratch_shapes=[
            pltpu.VMEM((T, D), bf16), pltpu.VMEM((T, D), bf16), pltpu.VMEM((T, D), bf16), pltpu.VMEM((T, D), bf16),
            pltpu.VMEM((C, D), f32),
            pltpu.VMEM((TM, C), bf16), pltpu.VMEM((TM, 2 * C), bf16),
            pltpu.VMEM((4, 2 * RB, C), bf16), pltpu.VMEM((2, C, D), bf16),
            pltpu.VMEM((2, 2 * RB, C), bf16), pltpu.VMEM((2, DH, D), bf16),
            pltpu.VMEM((4, 2 * RB, C), bf16), pltpu.VMEM((2, 2, DH, D), bf16),
            pltpu.VMEM((8, D), f32), pltpu.VMEM((4, 8, 128), f32), pltpu.VMEM((8, 128), f32),
            dma(L, 10, 4), dma(L, 10, 4), dma(L, 3), dma(L, 3), dma(2), dma(2, 7),
            dma(2), dma(2), dma(2, 2), dma(2), dma(L, 4), dma(L), dma(2), dma(4), dma(L, 4), dma(L, 2), dma(L, 2),
            dma(3), dma(2), dma(3), dma(4), dma(2, 2), dma(2), dma(3, 4), dma(3, 4),
        ],
        compiler_params=pltpu.CompilerParams(
            collective_id=0, has_side_effects=True, vmem_limit_bytes=MEGA * 2**20
        ),
        name="train_step",
    )(x, dy, *w, *m)


def adamw_kernel(*refs):
    fac, ins, outs = refs[0], refs[1:13], refs[13:]
    factor = fac[0:1, 0:1]
    for n in range(3):
        g, w, m, v = (ins[3 * which + n] for which in range(4))
        shape = g.shape[1:]
        grad = g[0].astype(f32) * factor
        new_m = 0.9 * m[...].reshape(shape) + 0.1 * grad
        new_v = 0.95 * v[0] + 0.05 * grad * grad
        wide = w[0].astype(f32)
        outs[n][0] = (wide - 0.02 * (new_m * lax.rsqrt(new_v + 1e-8) + 0.1 * wide)).astype(bf16)
        outs[3 + n][0] = new_m
        outs[6 + n][0] = new_v


def adamw(factor, g, v, m_down, m_gate, m_up, w_gu, w_d):
    n = 2
    rows, tall = RB // n, C // (2 * n)
    half = (rows, 2 * C)
    wide = pl.BlockSpec((1, *half), lambda t: (t // (2 * n), t % n, t // n % 2))
    down = pl.BlockSpec((1, tall, D), lambda t: (t // (2 * n), t % (2 * n), 0))
    w_at = lambda which: pl.BlockSpec((1, *half), lambda t: (which, t, 0))
    specs = [wide, wide, down]
    shapes = lambda dtype: [jax.ShapeDtypeStruct(a.shape, dtype) for a in v]
    return pl.pallas_call(
        adamw_kernel,
        grid=(2 * n * L,),
        in_specs=[pl.BlockSpec((8, 128), lambda t: (0, 0))]
        + specs
        + [w_at(0), w_at(1), down]
        + [
            pl.BlockSpec(half, lambda t: (t, 0)),
            pl.BlockSpec((1, *half), lambda t: (t // (2 * n), t % (2 * n), 0)),
            pl.BlockSpec((tall, D), lambda t: (t, 0)),
        ]
        + specs,
        out_specs=specs * 3,
        out_shape=shapes(bf16) + shapes(f32) + shapes(f32),
        compiler_params=pltpu.CompilerParams(vmem_limit_bytes=ADAMW * 2**20),
        name="adamw",
    )(factor, *g, *(pltpu.with_memory_space_constraint(a, pltpu.VMEM) for a in (w_gu, w_gu, w_d, m_gate, m_up, m_down)), *v)


def solution(mesh):
    def step(x, dy, *arrays):
        w, m, v = (arrays[n : n + 3] for n in (0, 3, 6))
        gg, gu, gd, factor, *rest = gradients(x[0], dy[0], w, m)
        return tuple(adamw(factor, (gg, gu, gd), v, *rest[-5:]))

    states, cut = P(("rep", "dp"), None, None), P(None, "dp", None)
    return jax.shard_map(
        step,
        mesh=mesh,
        in_specs=(states, states) + (cut,) * 9,
        out_specs=(P("rep", "dp", None),) * 9,
        check_vma=False,
    )
```
